32 devices in a mesh: dp: 2 (over x), col: 4 (over z), row: 4 (over y, core).
Axes of the slice: x: 2, y: 2, z: 4, core: 2. Of those that a mesh axis runs over, the one named last changes fastest.
Arguments:
- h_first: bfloat16 [64, 1024], P(('dp', 'col', 'row')), parts along dimension 0
- h_second: bfloat16 [64, 1024], P(('dp', 'col', 'row')), parts along dimension 0
- start_pos: int32 [64], P(('dp', 'col', 'row')), parts along dimension 0
- enc_lens: int32 [64], P(('dp', 'col', 'row')), parts along dimension 0
- dec_bias: float32 [32, 16], replicated
- norm_self: bfloat16 [2, 1024], replicated
- norm_cross: bfloat16 [2, 1024], replicated
- norm_mlp: bfloat16 [2, 1024], replicated
- w_query: bfloat16 [2, 1024, 1024], P(None, 'row', 'col')
- w_key: bfloat16 [2, 1024, 1024], P(None, 'row', 'col')
- w_value: bfloat16 [2, 1024, 1024], P(None, 'row', 'col')
- w_out: bfloat16 [2, 1024, 1024], P(None, 'row', 'col')
- w_cquery: bfloat16 [2, 1024, 1024], P(None, 'row', 'col')
- w_cout: bfloat16 [2, 1024, 1024], P(None, 'row', 'col')
- w_gate: bfloat16 [2, 1024, 2816], P(None, 'row', 'col')
- w_up: bfloat16 [2, 1024, 2816], P(None, 'row', 'col')
- w_down: bfloat16 [2, 2816, 1024], P(None, 'row', 'col')
- self_k: bfloat16 [2, 64, 1024, 16, 64], P(None, ('dp', 'col', 'row')), parts along dimension 1
- self_v: bfloat16 [2, 64, 1024, 16, 64], P(None, ('dp', 'col', 'row')), parts along dimension 1
- cross_k: bfloat16 [2, 64, 512, 16, 64], P(None, ('dp', 'col', 'row')), parts along dimension 1
- cross_v: bfloat16 [2, 64, 512, 16, 64], P(None, ('dp', 'col', 'row')), parts along dimension 1
Outputs:
- output 1: bfloat16 [2, 64, 1024], P(None, ('dp', 'col', 'row')), parts along dimension 1
- output 2: bfloat16 [2, 64, 1024, 16, 64], P(None, ('dp', 'col', 'row')), parts along dimension 1
- output 3: bfloat16 [2, 64, 1024, 16, 64], P(None, ('dp', 'col', 'row')), parts along dimension 1
There are 2 independent parts. The reference program is written for one: setup_inputs(seed, part) draws one part's arguments, and reference() takes and returns one part's arrays. A program takes and returns all parts, laid end to end along the dimension named above; an argument that names none is the same for every part.
All inputs are finite; a program needn't handle non-finite values.
Results may differ from the reference program's by a relative error of at most 0.0177046.
Values are sent between devices in bfloat16 or wider.
A program may use at most 1 GiB of HBM per device.

```python
import jax
import jax.numpy as jnp
from jax import lax

D_MODEL = 1024
HEADS = 16
HEAD_DIM = 64
D_FF = 2816
BATCH_SIZE = 32
CACHE_LEN = 1024
ENC_LEN = 512
NUM_LAYERS = 2
NUM_BUCKETS = 32

INNER_DIM = HEADS * HEAD_DIM
NORM_EPS = 1e-6
BUCKET_EDGES = (16, 19, 21, 24, 27, 31, 35, 40, 46, 52, 59, 67, 77, 87, 99, 113)


def setup_inputs(seed: int = 0, part: int = 0) -> dict:
    part_keys = jax.random.split(jax.random.fold_in(jax.random.key(seed), part), 8)
    shared_keys = jax.random.split(jax.random.key(seed + 1), 13)

    def normal_bf16(key, shape, scale):
        return (jax.random.normal(key, shape, jnp.float32) * scale).astype(jnp.bfloat16)

    def gain_draw(key):
        return jax.random.uniform(key, (NUM_LAYERS, D_MODEL), jnp.float32, 0.5, 1.5).astype(jnp.bfloat16)

    start_pos = jax.random.randint(part_keys[2], (BATCH_SIZE,), 0, CACHE_LEN - 1, jnp.int32)
    start_pos = start_pos.at[0].set(CACHE_LEN - 2).at[1].set(0)
    enc_lens = jax.random.randint(part_keys[3], (BATCH_SIZE,), 1, ENC_LEN + 1, jnp.int32)
    enc_lens = enc_lens.at[0].set(ENC_LEN).at[1].set(1)
    self_shape = (NUM_LAYERS, BATCH_SIZE, CACHE_LEN, HEADS, HEAD_DIM)
    cross_shape = (NUM_LAYERS, BATCH_SIZE, ENC_LEN, HEADS, HEAD_DIM)
    in_shape = (NUM_LAYERS, D_MODEL, INNER_DIM)
    out_shape = (NUM_LAYERS, INNER_DIM, D_MODEL)
    ff_shape = (NUM_LAYERS, D_MODEL, D_FF)
    down_shape = (NUM_LAYERS, D_FF, D_MODEL)
    query_scale = 1.5 * (D_MODEL * HEAD_DIM) ** -0.5
    model_scale = D_MODEL ** -0.5
    inner_scale = 2.0 * INNER_DIM ** -0.5
    return dict(
        h_first=normal_bf16(part_keys[0], (BATCH_SIZE, D_MODEL), 1.0),
        h_second=normal_bf16(part_keys[1], (BATCH_SIZE, D_MODEL), 1.0),
        start_pos=start_pos,
        enc_lens=enc_lens,
        dec_bias=jax.random.normal(shared_keys[0], (NUM_BUCKETS, HEADS), jnp.float32),
        norm_self=gain_draw(shared_keys[1]),
        norm_cross=gain_draw(shared_keys[2]),
        norm_mlp=gain_draw(shared_keys[3]),
        w_query=normal_bf16(shared_keys[4], in_shape, query_scale),
        w_key=normal_bf16(shared_keys[5], in_shape, model_scale),
        w_value=normal_bf16(shared_keys[6], in_shape, model_scale),
        w_out=normal_bf16(shared_keys[7], out_shape, inner_scale),
        w_cquery=normal_bf16(shared_keys[8], in_shape, query_scale),
        w_cout=normal_bf16(shared_keys[9], out_shape, inner_scale),
        w_gate=normal_bf16(shared_keys[10], ff_shape, model_scale),
        w_up=normal_bf16(shared_keys[11], ff_shape, model_scale),
        w_down=normal_bf16(shared_keys[12], down_shape, 1.5 * D_FF ** -0.5),
        self_k=normal_bf16(part_keys[4], self_shape, 1.0),
        self_v=normal_bf16(part_keys[5], self_shape, 1.0),
        cross_k=normal_bf16(part_keys[6], cross_shape, 1.0),
        cross_v=normal_bf16(part_keys[7], cross_shape, 1.0),
    )


def rms_norm(hidden, gain):
    mean_sq = jnp.mean(hidden * hidden, axis=-1, keepdims=True)
    return (hidden * lax.rsqrt(mean_sq + NORM_EPS) * gain.astype(jnp.float32)).astype(jnp.bfloat16)


def project(act, weight):
    return jnp.dot(act, weight, preferred_element_type=jnp.float32).astype(jnp.bfloat16)


def attend(query_vec, keys, values, bias):
    scores = jnp.einsum('bhd,bthd->bth', query_vec.astype(jnp.float32), keys.astype(jnp.float32)) + bias
    attn_probs = jax.nn.softmax(scores, axis=1).astype(jnp.bfloat16)
    mixed = jnp.einsum('bth,bthd->bhd', attn_probs.astype(jnp.float32), values.astype(jnp.float32))
    return mixed.astype(jnp.bfloat16).reshape(query_vec.shape[0], -1)


def position_bias(dec_bias, pos):
    offset = pos[:, None] - jnp.arange(CACHE_LEN, dtype=jnp.int32)[None, :]
    distance = jnp.maximum(offset, 0)
    bucket_edges = jnp.array(BUCKET_EDGES, dtype=jnp.int32)
    far_bucket = BUCKET_EDGES[0] - 1 + jnp.sum((distance[:, :, None] >= bucket_edges).astype(jnp.int32), axis=-1)
    bucket = jnp.where(distance < BUCKET_EDGES[0], distance, far_bucket)
    return jnp.where((offset >= 0)[:, :, None], dec_bias[bucket], -jnp.inf)


def cross_bias(enc_lens):
    in_range = jnp.arange(ENC_LEN, dtype=jnp.int32)[None, :, None] < enc_lens[:, None, None]
    return jnp.where(in_range, 0.0, -jnp.inf)


def decode_step(hidden, pos, enc_lens, dec_bias, layer_params):
    self_mask = position_bias(dec_bias, pos)
    cross_mask = cross_bias(enc_lens)
    write_mask = (jnp.arange(CACHE_LEN, dtype=jnp.int32)[None, :] == pos[:, None])[:, :, None, None]

    def layer_body(residual, params):
        (g_self, g_cross, g_mlp, w_query, w_key, w_value, w_out, w_cquery, w_cout,
         w_gate, w_up, w_down, keys_self, vals_self, keys_cross, vals_cross) = params
        normed = rms_norm(residual, g_self)
        query_vec = project(normed, w_query).reshape(-1, HEADS, HEAD_DIM)
        key_row = project(normed, w_key).reshape(-1, 1, HEADS, HEAD_DIM)
        val_row = project(normed, w_value).reshape(-1, 1, HEADS, HEAD_DIM)
        keys_self = jnp.where(write_mask, key_row, keys_self)
        vals_self = jnp.where(write_mask, val_row, vals_self)
        attn_out = attend(query_vec, keys_self, vals_self, self_mask)
        residual = residual + project(attn_out, w_out).astype(jnp.float32)
        normed = rms_norm(residual, g_cross)
        query_vec = project(normed, w_cquery).reshape(-1, HEADS, HEAD_DIM)
        attn_out = attend(query_vec, keys_cross, vals_cross, cross_mask)
        residual = residual + project(attn_out, w_cout).astype(jnp.float32)
        normed = rms_norm(residual, g_mlp)
        gate_val = project(normed, w_gate)
        up_val = project(normed, w_up)
        mlp_act = (jax.nn.silu(gate_val.astype(jnp.float32)) * up_val.astype(jnp.float32)).astype(jnp.bfloat16)
        residual = residual + project(mlp_act, w_down).astype(jnp.float32)
        return residual, (keys_self, vals_self)

    residual, (keys_all, vals_all) = lax.scan(layer_body, hidden.astype(jnp.float32), layer_params)
    return residual.astype(jnp.bfloat16), keys_all, vals_all


def reference(h_first, h_second, start_pos, enc_lens, dec_bias, norm_self, norm_cross, norm_mlp,
              w_query, w_key, w_value, w_out, w_cquery, w_cout, w_gate, w_up, w_down,
              self_k, self_v, cross_k, cross_v):
    shared = (norm_self, norm_cross, norm_mlp, w_query, w_key, w_value, w_out, w_cquery, w_cout,
              w_gate, w_up, w_down)
    first_out, keys_one, vals_one = decode_step(h_first, start_pos, enc_lens, dec_bias,
                                                shared + (self_k, self_v, cross_k, cross_v))
    second_out, keys_two, vals_two = decode_step(h_second, start_pos + 1, enc_lens, dec_bias,
                                                 shared + (keys_one, vals_one, cross_k, cross_v))
    return (jnp.stack([first_out, second_out]), keys_two, vals_two)
```

```python
import functools

import jax
import jax.numpy as jnp
from jax import lax
from jax.experimental import pallas as pl
from jax.experimental.pallas import tpu as pltpu
from jax.sharding import PartitionSpec as P

NORM_EPS = 1e-6
BUCKET_EDGES = (16, 19, 21, 24, 27, 31, 35, 40, 46, 52, 59, 67, 77, 87, 99, 113)
BUCKET_STARTS = tuple(range(16)) + BUCKET_EDGES
F32 = jnp.float32
BF16 = jnp.bfloat16
LAYERS = 2
SEQS = 2
TOK = 4
COLS = 4
ROWS = 4
PEERS = 16
D = 1024
HEADS = 16
T = 1024
E = 512
FB = 704
NEG = float("-inf")


def nt_dot(a, b):
    return lax.dot_general(a, b, (((1,), (1,)), ((), ())), preferred_element_type=F32)


def nn_dot(a, b):
    return jnp.dot(a, b, preferred_element_type=F32)


def body(h0_ref, h1_ref, pos_ref, len_ref, bias_ref, gs_ref, gc_ref, gm_ref,
         wq_ref, wk_ref, wv_ref, wo_ref, wcq_ref, wco_ref, wg_ref, wu_ref, wd_ref,
         sk_hbm, sv_hbm, ck_hbm, cv_hbm,
         hid_ref, krow_ref, vrow_ref,
         sk, sv, ck, cv, self_bias,
         a_send, a_recv, a_mat, p3_send, p3_recv, p1_send, p1_recv,
         gu_send, gu_recv, u_send, u_recv, u_mat,
         cache_sem, send_sem, recv_sem):
    col = lax.axis_index('col')
    row = lax.axis_index('row')
    me = col * ROWS + row

    def peer_of(k):
        other = lax.rem(me + k, PEERS)
        return other, other // ROWS, lax.rem(other, ROWS)

    cache_copies = []
    for l in range(LAYERS):
        for i, (src, dst) in enumerate(((sk_hbm, sk), (sv_hbm, sv), (ck_hbm, ck), (cv_hbm, cv))):
            cp = pltpu.make_async_copy(src.at[l], dst.at[l], cache_sem.at[l, i])
            cp.start()
            cache_copies.append(cp)

    barrier = pltpu.get_barrier_semaphore()
    for k in range(1, PEERS):
        _, c, r = peer_of(k)
        pl.semaphore_signal(barrier, inc=1, device_id={'col': c, 'row': r}, device_id_type=pl.DeviceIdType.MESH)
    pl.semaphore_wait(barrier, PEERS - 1)

    def exchange(send, recv, idx, by_row):
        for k in range(1, PEERS):
            other, c, r = peer_of(k)
            pltpu.make_async_remote_copy(
                src_ref=send.at[r if by_row else other], dst_ref=recv.at[me],
                send_sem=send_sem.at[idx], recv_sem=recv_sem.at[idx],
                device_id={'col': c, 'row': r}, device_id_type=pl.DeviceIdType.MESH).start()
        recv[me] = send[row if by_row else me]

    def arrive(recv, idx):
        part = recv.at[pl.ds(0, PEERS - 1)]
        pltpu.make_async_copy(part, part, recv_sem.at[idx]).wait()

    def left(recv, idx):
        part = recv.at[pl.ds(0, PEERS - 1)]
        pltpu.make_async_copy(part, part, send_sem.at[idx]).wait()

    jpos = lax.broadcasted_iota(jnp.int32, (HEADS, T), 1)
    for b in range(SEQS):
        p = pos_ref[b]
        for t in range(2):
            dist = p + t - jpos
            val = jnp.broadcast_to(bias_ref[:, 0:1], (HEADS, T))
            for n in range(1, 32):
                val = jnp.where(dist >= BUCKET_STARTS[n], bias_ref[:, n:n + 1], val)
            self_bias[b, pl.ds(t * HEADS, HEADS), :] = jnp.where(jpos < p, val, NEG)

    r32 = lax.broadcasted_iota(jnp.int32, (32, 8), 0)
    c8 = lax.broadcasted_iota(jnp.int32, (32, 8), 1)
    db0 = jnp.concatenate([bias_ref[:, 0:1]] * 2, axis=0)
    db1 = jnp.concatenate([bias_ref[:, 1:2]] * 2, axis=0)
    new_bias = jnp.where(c8 == 0, jnp.where(r32 < HEADS, db0, db1),
                         jnp.where((c8 == 1) & (r32 >= HEADS), db0, NEG))
    head_of = (lax.broadcasted_iota(jnp.int32, (32, D), 1) // 64) == lax.rem(
        lax.broadcasted_iota(jnp.int32, (32, D), 0), HEADS)
    jcross = lax.broadcasted_iota(jnp.int32, (32, E), 1)

    def rms(x, gain):
        mean_sq = jnp.mean(x * x, axis=-1, keepdims=True)
        return x * lax.rsqrt(mean_sq + NORM_EPS) * gain.astype(F32)

    def put_act(vec, l, e):
        for r in range(ROWS):
            a_send[l, e, r] = vec[:, r * 256:(r + 1) * 256]

    def gather_act(recv, mat):
        rows = jnp.concatenate([recv[s].astype(F32) for s in range(PEERS)], axis=0)
        return rows.astype(BF16)

    def spread_query(q4, b):
        q_first = jnp.broadcast_to(q4[b:b + 1, :], (HEADS, D))
        q_second = jnp.broadcast_to(q4[2 + b:3 + b, :], (HEADS, D))
        q = jnp.concatenate([q_first, q_second], axis=0)
        return jnp.where(head_of, q, 0.0).astype(BF16)

    def fold_heads(mixed):
        keep = jnp.where(head_of, mixed, 0.0)
        return (jnp.sum(keep[:HEADS], axis=0, keepdims=True), jnp.sum(keep[HEADS:], axis=0, keepdims=True))

    def join_tokens(pieces):
        return jnp.concatenate([pieces[0][0], pieces[1][0], pieces[0][1], pieces[1][1]], axis=0)

    def row_sum(get):
        return [(get(c * ROWS) + get(c * ROWS + 1)) + (get(c * ROWS + 2) + get(c * ROWS + 3)) for c in range(COLS)]

    def round_bf16(v):
        return v.astype(BF16).astype(F32)

    def project(vec, weight, l, e, slot):
        put_act(vec, l, e)
        exchange(a_send.at[l, e], a_recv.at[l, e], l * 12 + slot, True)
        arrive(a_recv.at[l, e], l * 12 + slot)
        prod = nn_dot(gather_act(a_recv.at[l, e], a_mat), weight)
        for s in range(PEERS):
            p1_send[l, e - 1, s] = prod[s * TOK:(s + 1) * TOK, :]
        exchange(p1_send.at[l, e - 1], p1_recv.at[l, e - 1], l * 12 + slot + 1, False)
        arrive(p1_recv.at[l, e - 1], l * 12 + slot + 1)
        sums = row_sum(lambda s: p1_recv[l, e - 1, s])
        return round_bf16(jnp.concatenate(sums, axis=1))

    x = jnp.concatenate([h0_ref[...].astype(F32), h1_ref[...].astype(F32)], axis=0)
    for l in range(LAYERS):
        base = l * 12
        n = rms(x, gs_ref[l:l + 1, :]).astype(BF16)
        put_act(n, l, 0)
        exchange(a_send.at[l, 0], a_recv.at[l, 0], base, True)
        arrive(a_recv.at[l, 0], base)
        act = gather_act(a_recv.at[l, 0], a_mat)
        for i, w in enumerate((wq_ref, wk_ref, wv_ref)):
            prod = nn_dot(act, w[l])
            for s in range(PEERS):
                p3_send[l, s, :, i * 256:(i + 1) * 256] = prod[s * TOK:(s + 1) * TOK, :]
        exchange(p3_send.at[l], p3_recv.at[l], base + 1, False)
        arrive(p3_recv.at[l], base + 1)
        sums = row_sum(lambda s: p3_recv[l, s])
        q4, k4, v4 = (round_bf16(jnp.concatenate([sm[:, i * 256:(i + 1) * 256] for sm in sums], axis=1))
                      for i in range(3))
        krow_ref[l] = k4
        vrow_ref[l] = v4
        if True:
            cache_copies[l * 4].wait()
            cache_copies[l * 4 + 1].wait()
        pieces = []
        for b in range(SEQS):
            qb = spread_query(q4, b)
            zeros = jnp.zeros((6, D), F32)
            kn = jnp.concatenate([k4[b:b + 1], k4[2 + b:3 + b], zeros], axis=0).astype(BF16)
            vn = jnp.concatenate([v4[b:b + 1], v4[2 + b:3 + b], zeros], axis=0).astype(BF16)
            old = nn_dot(qb, sk[l, b]) + self_bias[b]
            new = nt_dot(qb, kn) + new_bias
            top = jnp.maximum(jnp.max(old, axis=1, keepdims=True), jnp.max(new, axis=1, keepdims=True))
            e_old = jnp.exp(old - top)
            e_new = jnp.exp(new - top)
            total = jnp.sum(e_old, axis=1, keepdims=True) + jnp.sum(e_new, axis=1, keepdims=True)
            mixed = nt_dot((e_old / total).astype(BF16), sv[l, b]) + nn_dot((e_new / total).astype(BF16), vn)
            pieces.append(fold_heads(mixed))
        x = x + project(join_tokens(pieces).astype(BF16), wo_ref[l], l, 1, 2)

        n = rms(x, gc_ref[l:l + 1, :]).astype(BF16)
        q4 = project(n, wcq_ref[l], l, 2, 4)
        cache_copies[l * 4 + 2].wait()
        cache_copies[l * 4 + 3].wait()
        pieces = []
        for b in range(SEQS):
            qb = spread_query(q4, b)
            sc = jnp.where(jcross < len_ref[b], nn_dot(qb, ck[l, b]), NEG)
            ex = jnp.exp(sc - jnp.max(sc, axis=1, keepdims=True))
            probs = (ex / jnp.sum(ex, axis=1, keepdims=True)).astype(BF16)
            pieces.append(fold_heads(nt_dot(probs, cv[l, b])))
        x = x + project(join_tokens(pieces).astype(BF16), wco_ref[l], l, 3, 6)

        n = rms(x, gm_ref[l:l + 1, :]).astype(BF16)
        put_act(n, l, 4)
        exchange(a_send.at[l, 4], a_recv.at[l, 4], base + 8, True)
        arrive(a_recv.at[l, 4], base + 8)
        act = gather_act(a_recv.at[l, 4], a_mat)
        for i, w in enumerate((wg_ref, wu_ref)):
            prod = nt_dot(act, w[l])
            for s in range(PEERS):
                gu_send[l, s, pl.ds(i * TOK, TOK), :] = prod[s * TOK:(s + 1) * TOK, :]
        exchange(gu_send.at[l], gu_recv.at[l], base + 9, False)
        arrive(gu_recv.at[l], base + 9)
        sums = row_sum(lambda s: gu_recv[l, s])
        for c in range(COLS):
            gate = round_bf16(sums[c][:TOK])
            up = round_bf16(sums[c][TOK:])
            u_send[l, c] = (jax.nn.silu(gate) * up).astype(BF16)
        exchange(u_send.at[l], u_recv.at[l], base + 10, True)
        arrive(u_recv.at[l], base + 10)
        prod = nn_dot(gather_act(u_recv.at[l], u_mat), wd_ref[l])
        for s in range(PEERS):
            p1_send[l, 3, s] = prod[s * TOK:(s + 1) * TOK, :]
        exchange(p1_send.at[l, 3], p1_recv.at[l, 3], base + 11, False)
        arrive(p1_recv.at[l, 3], base + 11)
        sums = row_sum(lambda s: p1_recv[l, 3, s])
        x = x + round_bf16(jnp.concatenate(sums, axis=1))

    hid_ref[0] = x[0:2].astype(BF16)
    hid_ref[1] = x[2:4].astype(BF16)
    for l in range(LAYERS):
        base = l * 12
        left(a_recv.at[l, 0], base)
        left(p3_recv.at[l], base + 1)
        for e in (1, 2, 3):
            left(a_recv.at[l, e], base + 2 * e)
            left(p1_recv.at[l, e - 1], base + 2 * e + 1)
        left(a_recv.at[l, 4], base + 8)
        left(gu_recv.at[l], base + 9)
        left(u_recv.at[l], base + 10)
        left(p1_recv.at[l, 3], base + 11)


def decode(*args):
    vmem = pl.BlockSpec(memory_space=pltpu.VMEM)
    smem = pl.BlockSpec(memory_space=pltpu.SMEM)
    hbm = pl.BlockSpec(memory_space=pl.ANY)
    return pl.pallas_call(
        body,
        out_shape=(jax.ShapeDtypeStruct((2, SEQS, D), BF16),
                   jax.ShapeDtypeStruct((LAYERS, TOK, D), F32),
                   jax.ShapeDtypeStruct((LAYERS, TOK, D), F32)),
        in_specs=[vmem, vmem, smem, smem] + [vmem] * 13 + [hbm] * 4,
        out_specs=(vmem,) * 3,
        scratch_shapes=[
            pltpu.VMEM((LAYERS, SEQS, D, T), BF16),
            pltpu.VMEM((LAYERS, SEQS, D, T), BF16),
            pltpu.VMEM((LAYERS, SEQS, D, E), BF16),
            pltpu.VMEM((LAYERS, SEQS, D, E), BF16),
            pltpu.VMEM((SEQS, 32, T), F32),
            pltpu.VMEM((LAYERS, 5, ROWS, TOK, 256), BF16),
            pltpu.VMEM((LAYERS, 5, PEERS, TOK, 256), BF16),
            pltpu.VMEM((PEERS * TOK, 256), BF16),
            pltpu.VMEM((LAYERS, PEERS, TOK, 768), F32),
            pltpu.VMEM((LAYERS, PEERS, TOK, 768), F32),
            pltpu.VMEM((LAYERS, 4, PEERS, TOK, 256), F32),
            pltpu.VMEM((LAYERS, 4, PEERS, TOK, 256), F32),
            pltpu.VMEM((LAYERS, PEERS, 2 * TOK, FB), F32),
            pltpu.VMEM((LAYERS, PEERS, 2 * TOK, FB), F32),
            pltpu.VMEM((LAYERS, COLS, TOK, FB), BF16),
            pltpu.VMEM((LAYERS, PEERS, TOK, FB), BF16),
            pltpu.VMEM((PEERS * TOK, FB), BF16),
            pltpu.SemaphoreType.DMA((LAYERS, 4)),
            pltpu.SemaphoreType.DMA((LAYERS * 12,)),
            pltpu.SemaphoreType.DMA((LAYERS * 12,)),
        ],
        compiler_params=pltpu.CompilerParams(collective_id=0, has_side_effects=True,
                                             vmem_limit_bytes=60 * 1024 * 1024),
    )(*args)


def solution(mesh):
    batch_axes = ('dp', 'col', 'row')

    def local_step(h_first, h_second, start_pos, enc_lens, dec_bias, norm_self, norm_cross, norm_mlp,
                   w_query, w_key, w_value, w_out, w_cquery, w_cout, w_gate, w_up, w_down,
                   self_k, self_v, cross_k, cross_v):
        def flat(cache):
            l, b, t, h, d = cache.shape
            return cache.transpose(0, 1, 3, 4, 2).reshape(l, b, h * d, t)

        hidden, krows, vrows = decode(
            h_first, h_second, start_pos, enc_lens, dec_bias.T, norm_self, norm_cross, norm_mlp,
            w_query, w_key, w_value, w_out, w_cquery, w_cout,
            w_gate.transpose(0, 2, 1), w_up.transpose(0, 2, 1), w_down,
            flat(self_k), flat(self_v), flat(cross_k), flat(cross_v))

        at = jnp.arange(T, dtype=jnp.int32)[None, None, :, None, None]
        first = at == start_pos[None, :, None, None, None]
        second = at == (start_pos + 1)[None, :, None, None, None]

        def write(cache, rows):
            rows = rows.astype(BF16).reshape(LAYERS, 2, SEQS, 1, HEADS, 64)
            return jnp.where(first, rows[:, 0], jnp.where(second, rows[:, 1], cache))

        return hidden, write(self_k, krows), write(self_v, vrows)

    row_spec = P(batch_axes, None)
    seq_spec = P(batch_axes)
    weight_spec = P(None, 'row', 'col')
    cache_spec = P(None, batch_axes)
    in_specs = (row_spec, row_spec, seq_spec, seq_spec, P(), P(), P(), P()) + (weight_spec,) * 9 + (cache_spec,) * 4
    out_specs = (P(None, batch_axes), cache_spec, cache_spec)
    return jax.shard_map(local_step, mesh=mesh, in_specs=in_specs, out_specs=out_specs, check_vma=False)
```

```python
import functools

import jax
import jax.numpy as jnp
from jax import lax
from jax.experimental import pallas as pl
from jax.experimental.pallas import tpu as pltpu
from jax.sharding import PartitionSpec as P

NORM_EPS = 1e-6
BUCKET_EDGES = (16, 19, 21, 24, 27, 31, 35, 40, 46, 52, 59, 67, 77, 87, 99, 113)
BUCKET_STARTS = tuple(range(16)) + BUCKET_EDGES
F32 = jnp.float32
BF16 = jnp.bfloat16
LAYERS = 2
SEQS = 2
TOK = 4
COLS = 4
ROWS = 4
PEERS = 16
D = 1024
HEADS = 16
T = 1024
E = 512
FB = 704
FS = 176
NEG = float("-inf")


def nt_dot(a, b):
    return lax.dot_general(a, b, (((1,), (1,)), ((), ())), preferred_element_type=F32)


def nn_dot(a, b):
    return jnp.dot(a, b, preferred_element_type=F32)


def body(h0_ref, h1_ref, pos_ref, len_ref, bias_ref, gs_ref, gc_ref, gm_ref,
         wq_hbm, wk_hbm, wv_hbm, wo_hbm, wcq_hbm, wco_hbm, wg_hbm, wu_hbm, wd_hbm,
         sk_hbm, sv_hbm, ck_hbm, cv_hbm,
         hid_ref, new_ref,
         sk, sv, ck, cv, self_bias, proj_w, gate_w, up_w, down_w,
         a_send, a_recv, p3_send, p3_recv, p1_send, p1_recv,
         n_send, n_recv, d_send, d_recv,
         cache_sem, weight_sem, mlp_send_sem, mlp_recv_sem, send_sem, recv_sem):
    col = lax.axis_index('col')
    row = lax.axis_index('row')
    me = col * ROWS + row

    def peer_of(k):
        other = lax.rem(me + k, PEERS)
        return other, other // ROWS, lax.rem(other, ROWS)

    weight_copies = []
    for i, src in enumerate((wq_hbm, wk_hbm, wv_hbm, wo_hbm, wcq_hbm, wco_hbm)):
        cp = pltpu.make_async_copy(src, proj_w.at[i], weight_sem.at[i])
        cp.start()
        weight_copies.append(cp)
    cache_copies = []
    for l in range(LAYERS):
        for i, (src, dst) in enumerate(((sk_hbm, sk), (sv_hbm, sv), (ck_hbm, ck), (cv_hbm, cv))):
            cp = pltpu.make_async_copy(src.at[l], dst.at[l], cache_sem.at[l, i])
            cp.start()
            cache_copies.append(cp)

    barrier = pltpu.get_barrier_semaphore()
    for k in range(1, PEERS):
        _, c, r = peer_of(k)
        pl.semaphore_signal(barrier, inc=1, device_id={'col': c, 'row': r}, device_id_type=pl.DeviceIdType.MESH)
    pl.semaphore_wait(barrier, PEERS - 1)

    def exchange(send, recv, idx, by_row):
        def pick(r, other):
            return 0 if by_row is None else (r if by_row else other)

        for k in range(1, PEERS):
            other, c, r = peer_of(k)
            pltpu.make_async_remote_copy(
                src_ref=send.at[pick(r, other)], dst_ref=recv.at[me],
                send_sem=send_sem.at[idx], recv_sem=recv_sem.at[idx],
                device_id={'col': c, 'row': r}, device_id_type=pl.DeviceIdType.MESH).start()
        recv[me] = send[pick(row, me)]

    def arrive(recv, idx):
        part = recv.at[pl.ds(0, PEERS - 1)]
        pltpu.make_async_copy(part, part, recv_sem.at[idx]).wait()

    def left(recv, idx):
        part = recv.at[pl.ds(0, PEERS - 1)]
        pltpu.make_async_copy(part, part, send_sem.at[idx]).wait()

    def build_bias():
        jpos = lax.broadcasted_iota(jnp.int32, (HEADS, T), 1)
        for b in range(SEQS):
            p = pos_ref[b]
            for t in range(2):
                dist = p + t - jpos
                val = jnp.broadcast_to(bias_ref[:, 0:1], (HEADS, T))
                for n in range(1, 32):
                    val = jnp.where(dist >= BUCKET_STARTS[n], bias_ref[:, n:n + 1], val)
                self_bias[b, pl.ds(t * HEADS, HEADS), :] = jnp.where(jpos < p, val, NEG)

    r32 = lax.broadcasted_iota(jnp.int32, (32, 8), 0)
    c8 = lax.broadcasted_iota(jnp.int32, (32, 8), 1)
    db0 = jnp.concatenate([bias_ref[:, 0:1]] * 2, axis=0)
    db1 = jnp.concatenate([bias_ref[:, 1:2]] * 2, axis=0)
    new_bias = jnp.where(c8 == 0, jnp.where(r32 < HEADS, db0, db1),
                         jnp.where((c8 == 1) & (r32 >= HEADS), db0, NEG))
    head_of = (lax.broadcasted_iota(jnp.int32, (32, D), 1) // 64) == lax.rem(
        lax.broadcasted_iota(jnp.int32, (32, D), 0), HEADS)
    jcross = lax.broadcasted_iota(jnp.int32, (32, E), 1)

    def rms(x, gain):
        mean_sq = jnp.mean(x * x, axis=-1, keepdims=True)
        return x * lax.rsqrt(mean_sq + NORM_EPS) * gain.astype(F32)

    def put_act(vec, l, e):
        for r in range(ROWS):
            a_send[l, e, r] = vec[:, r * 256:(r + 1) * 256]

    def gather_act(recv):
        rows = jnp.concatenate([recv[s].astype(F32) for s in range(PEERS)], axis=0)
        return rows.astype(BF16)

    def spread_query(q4, b):
        q_first = jnp.broadcast_to(q4[b:b + 1, :], (HEADS, D))
        q_second = jnp.broadcast_to(q4[2 + b:3 + b, :], (HEADS, D))
        q = jnp.concatenate([q_first, q_second], axis=0)
        return jnp.where(head_of, q, 0.0).astype(BF16)

    def fold_heads(mixed):
        keep = jnp.where(head_of, mixed, 0.0)
        return (jnp.sum(keep[:HEADS], axis=0, keepdims=True), jnp.sum(keep[HEADS:], axis=0, keepdims=True))

    def join_tokens(pieces):
        return jnp.concatenate([pieces[0][0], pieces[1][0], pieces[0][1], pieces[1][1]], axis=0)

    def row_sum(get):
        return [(get(c * ROWS) + get(c * ROWS + 1)) + (get(c * ROWS + 2) + get(c * ROWS + 3)) for c in range(COLS)]

    def round_bf16(v):
        return v.astype(BF16).astype(F32)

    def project(vec, which, l, e, slot):
        put_act(vec, l, e)
        exchange(a_send.at[l, e], a_recv.at[l, e], l * 10 + slot, True)
        arrive(a_recv.at[l, e], l * 10 + slot)
        prod = nn_dot(gather_act(a_recv.at[l, e]), proj_w[which, l])
        for s in range(PEERS):
            p1_send[l, e - 1, s] = prod[s * TOK:(s + 1) * TOK, :]
        exchange(p1_send.at[l, e - 1], p1_recv.at[l, e - 1], l * 10 + slot + 1, False)
        arrive(p1_recv.at[l, e - 1], l * 10 + slot + 1)
        sums = row_sum(lambda s: p1_recv[l, e - 1, s])
        return round_bf16(jnp.concatenate(sums, axis=1))

    def mlp_copies(l):
        for i, (src, dst) in enumerate(((wg_hbm, gate_w), (wu_hbm, up_w))):
            for k in range(ROWS):
                r = lax.rem(row + k, ROWS)
                part = src.at[l, pl.ds(pl.multiple_of(r * FS, 16), FS), :]
                if k == 0:
                    pltpu.make_async_copy(part, dst.at[l, row], mlp_recv_sem.at[l, i]).start()
                else:
                    pltpu.make_async_remote_copy(
                        src_ref=part, dst_ref=dst.at[l, row], send_sem=mlp_send_sem.at[l, i],
                        recv_sem=mlp_recv_sem.at[l, i], device_id={'col': col, 'row': r},
                        device_id_type=pl.DeviceIdType.MESH).start()
        for k in range(ROWS):
            r = lax.rem(row + k, ROWS)
            part = wd_hbm.at[l, pl.ds(pl.multiple_of(r * FS, 16), FS), :]

            def away():
                pltpu.make_async_remote_copy(
                    src_ref=part, dst_ref=down_w.at[l, col], send_sem=mlp_send_sem.at[l, 2],
                    recv_sem=mlp_recv_sem.at[l, 2], device_id={'col': row, 'row': r},
                    device_id_type=pl.DeviceIdType.MESH).start()

            if k == 0:
                pl.when(col != row)(away)

                @pl.when(col == row)
                def _():
                    pltpu.make_async_copy(part, down_w.at[l, col], mlp_recv_sem.at[l, 2]).start()
            else:
                away()

    def mlp_arrive(l):
        for i, dst in enumerate((gate_w, up_w, down_w)):
            pltpu.make_async_copy(dst.at[l], dst.at[l], mlp_recv_sem.at[l, i]).wait()

    def mlp_left(l):
        for i, dst in enumerate((gate_w, up_w, down_w)):
            part = dst.at[l, pl.ds(0, ROWS - 1)]
            pltpu.make_async_copy(part, part, mlp_send_sem.at[l, i]).wait()

        @pl.when(col != row)
        def _():
            part = down_w.at[l, 0]
            pltpu.make_async_copy(part, part, mlp_send_sem.at[l, 2]).wait()

    x = jnp.concatenate([h0_ref[...].astype(F32), h1_ref[...].astype(F32)], axis=0)
    for l in range(LAYERS):
        base = l * 10
        n = rms(x, gs_ref[l:l + 1, :]).astype(BF16)
        put_act(n, l, 0)
        exchange(a_send.at[l, 0], a_recv.at[l, 0], base, True)
        if l == 0:
            build_bias()
            for cp in weight_copies:
                cp.wait()
        arrive(a_recv.at[l, 0], base)
        act = gather_act(a_recv.at[l, 0])
        for i in range(3):
            prod = nn_dot(act, proj_w[i, l])
            for s in range(PEERS):
                p3_send[l, s, :, i * 256:(i + 1) * 256] = prod[s * TOK:(s + 1) * TOK, :]
        exchange(p3_send.at[l], p3_recv.at[l], base + 1, False)
        mlp_copies(l)
        arrive(p3_recv.at[l], base + 1)
        sums = row_sum(lambda s: p3_recv[l, s])
        q4, k4, v4 = (round_bf16(jnp.concatenate([sm[:, i * 256:(i + 1) * 256] for sm in sums], axis=1))
                      for i in range(3))
        new_ref[pl.ds(l * 8, TOK), :] = k4
        new_ref[pl.ds(l * 8 + TOK, TOK), :] = v4
        cache_copies[l * 4].wait()
        cache_copies[l * 4 + 1].wait()
        pieces = []
        for b in range(SEQS):
            qb = spread_query(q4, b)
            zeros = jnp.zeros((6, D), F32)
            kn = jnp.concatenate([k4[b:b + 1], k4[2 + b:3 + b], zeros], axis=0).astype(BF16)
            vn = jnp.concatenate([v4[b:b + 1], v4[2 + b:3 + b], zeros], axis=0).astype(BF16)
            old = nn_dot(qb, sk[l, b]) + self_bias[b]
            new = nt_dot(qb, kn) + new_bias
            top = jnp.maximum(jnp.max(old, axis=1, keepdims=True), jnp.max(new, axis=1, keepdims=True))
            e_old = jnp.exp(old - top)
            e_new = jnp.exp(new - top)
            total = jnp.sum(e_old, axis=1, keepdims=True) + jnp.sum(e_new, axis=1, keepdims=True)
            mixed = nt_dot((e_old / total).astype(BF16), sv[l, b]) + nn_dot((e_new / total).astype(BF16), vn)
            pieces.append(fold_heads(mixed))
        x = x + project(join_tokens(pieces).astype(BF16), 3, l, 1, 2)

        n = rms(x, gc_ref[l:l + 1, :]).astype(BF16)
        q4 = project(n, 4, l, 2, 4)
        cache_copies[l * 4 + 2].wait()
        cache_copies[l * 4 + 3].wait()
        pieces = []
        for b in range(SEQS):
            qb = spread_query(q4, b)
            sc = jnp.where(jcross < len_ref[b], nn_dot(qb, ck[l, b]), NEG)
            ex = jnp.exp(sc - jnp.max(sc, axis=1, keepdims=True))
            probs = (ex / jnp.sum(ex, axis=1, keepdims=True)).astype(BF16)
            pieces.append(fold_heads(nt_dot(probs, cv[l, b])))
        x = x + project(join_tokens(pieces).astype(BF16), 5, l, 3, 6)

        n_send[l, 0] = rms(x, gm_ref[l:l + 1, :]).astype(BF16)
        exchange(n_send.at[l], n_recv.at[l], base + 8, None)
        mlp_arrive(l)
        arrive(n_recv.at[l], base + 8)
        act = gather_act(n_recv.at[l])
        gate = nt_dot(act[:, 0:256], gate_w[l, 0])
        up = nt_dot(act[:, 0:256], up_w[l, 0])
        for r in range(1, ROWS):
            gate = gate + nt_dot(act[:, r * 256:(r + 1) * 256], gate_w[l, r])
            up = up + nt_dot(act[:, r * 256:(r + 1) * 256], up_w[l, r])
        u = (jax.nn.silu(round_bf16(gate)) * round_bf16(up)).astype(BF16)
        for c in range(COLS):
            prod = nn_dot(u, down_w[l, c])
            for s in range(PEERS):
                d_send[l, s, :, c * 256:(c + 1) * 256] = prod[s * TOK:(s + 1) * TOK, :]
        exchange(d_send.at[l], d_recv.at[l], base + 9, False)
        arrive(d_recv.at[l], base + 9)
        terms = [d_recv[l, s] for s in range(PEERS)]
        while len(terms) > 1:
            terms = [terms[i] + terms[i + 1] for i in range(0, len(terms), 2)]
        x = x + round_bf16(terms[0])

    hid_ref[0] = x[0:2].astype(BF16)
    hid_ref[1] = x[2:4].astype(BF16)
    for l in range(LAYERS):
        base = l * 10
        left(a_recv.at[l, 0], base)
        left(p3_recv.at[l], base + 1)
        for e in (1, 2, 3):
            left(a_recv.at[l, e], base + 2 * e)
            left(p1_recv.at[l, e - 1], base + 2 * e + 1)
        left(n_recv.at[l], base + 8)
        left(d_recv.at[l], base + 9)
        mlp_left(l)


def write_body(pos_ref, new_ref, k_ref, v_ref, ko_ref, vo_ref, cols):
    i = pl.program_id(0)
    half = pl.program_id(1)

    @pl.when((i == 0) & (half == 0))
    def _():
        cols[...] = jnp.transpose(new_ref[...])

    b = lax.rem(i, SEQS)
    l = i // SEQS
    p = pos_ref[b]
    lanes = lax.broadcasted_iota(jnp.int32, (512, 128), 1)
    pick = lax.broadcasted_iota(jnp.int32, (512, 16), 1)
    mine = cols[pl.ds(pl.multiple_of(half * 512, 512), 512), :]
    for kv, (src, dst) in enumerate(((k_ref, ko_ref), (v_ref, vo_ref))):
        dst[...] = src[...]
        at = l * 8 + kv * TOK + b
        first = jnp.sum(jnp.where(pick == at, mine, 0.0), axis=1, keepdims=True)
        second = jnp.sum(jnp.where(pick == at + 2, mine, 0.0), axis=1, keepdims=True)
        for q in range(2):
            start = pl.multiple_of(((p + q) // 128) * 128, 128)
            old = src[0, 0, :, pl.ds(start, 128)].astype(F32)
            fresh = jnp.where(lanes + start == p, first, jnp.where(lanes + start == p + 1, second, old))
            dst[0, 0, :, pl.ds(start, 128)] = fresh.astype(BF16)


def write_caches(pos, new, k, v):
    block = pl.BlockSpec((1, 1, 512, T), lambda i, j: (i // SEQS, i % SEQS, j, 0))
    return pl.pallas_call(
        write_body,
        grid=(LAYERS * SEQS, 2),
        out_shape=(jax.ShapeDtypeStruct(k.shape, BF16),) * 2,
        in_specs=[pl.BlockSpec(memory_space=pltpu.SMEM), pl.BlockSpec((16, D), lambda i, j: (0, 0)), block, block],
        out_specs=(block, block),
        scratch_shapes=[pltpu.VMEM((D, 16), F32)],
        compiler_params=pltpu.CompilerParams(vmem_limit_bytes=14 * 1024 * 1024),
        cost_estimate=pl.CostEstimate(flops=1000000, bytes_accessed=32 << 20, transcendentals=0),
    )(pos, new, k, v)


def decode(*args):
    vmem = pl.BlockSpec(memory_space=pltpu.VMEM)
    smem = pl.BlockSpec(memory_space=pltpu.SMEM)
    hbm = pl.BlockSpec(memory_space=pltpu.HBM)
    args = tuple(pltpu.with_memory_space_constraint(a, pltpu.HBM) for a in args)
    return pl.pallas_call(
        body,
        out_shape=(jax.ShapeDtypeStruct((2, SEQS, D), BF16),
                   jax.ShapeDtypeStruct((16, D), F32)),
        in_specs=[vmem, vmem, smem, smem] + [vmem] * 4 + [hbm] * 13,
        out_specs=(vmem,) * 2,
        scratch_shapes=[
            pltpu.VMEM((LAYERS, SEQS, D, T), BF16),
            pltpu.VMEM((LAYERS, SEQS, D, T), BF16),
            pltpu.VMEM((LAYERS, SEQS, D, E), BF16),
            pltpu.VMEM((LAYERS, SEQS, D, E), BF16),
            pltpu.VMEM((SEQS, 32, T), F32),
            pltpu.VMEM((6, LAYERS, 256, 256), BF16),
            pltpu.VMEM((LAYERS, ROWS, FS, 256), BF16),
            pltpu.VMEM((LAYERS, ROWS, FS, 256), BF16),
            pltpu.VMEM((LAYERS, COLS, FS, 256), BF16),
            pltpu.VMEM((LAYERS, 4, ROWS, TOK, 256), BF16),
            pltpu.VMEM((LAYERS, 4, PEERS, TOK, 256), BF16),
            pltpu.VMEM((LAYERS, PEERS, TOK, 768), F32),
            pltpu.VMEM((LAYERS, PEERS, TOK, 768), F32),
            pltpu.VMEM((LAYERS, 3, PEERS, TOK, 256), F32),
            pltpu.VMEM((LAYERS, 3, PEERS, TOK, 256), F32),
            pltpu.VMEM((LAYERS, 1, TOK, D), BF16),
            pltpu.VMEM((LAYERS, PEERS, TOK, D), BF16),
            pltpu.VMEM((LAYERS, PEERS, TOK, D), F32),
            pltpu.VMEM((LAYERS, PEERS, TOK, D), F32),
            pltpu.SemaphoreType.DMA((LAYERS, 4)),
            pltpu.SemaphoreType.DMA((6,)),
            pltpu.SemaphoreType.DMA((LAYERS, 3)),
            pltpu.SemaphoreType.DMA((LAYERS, 3)),
            pltpu.SemaphoreType.DMA((LAYERS * 10,)),
            pltpu.SemaphoreType.DMA((LAYERS * 10,)),
        ],
        compiler_params=pltpu.CompilerParams(collective_id=0, has_side_effects=True,
                                             vmem_limit_bytes=44 * 1024 * 1024),
        cost_estimate=pl.CostEstimate(flops=400000000, bytes_accessed=32 << 20, transcendentals=0),
    )(*args)


def solution(mesh):
    batch_axes = ('dp', 'col', 'row')

    def local_step(h_first, h_second, start_pos, enc_lens, dec_bias, norm_self, norm_cross, norm_mlp,
                   w_query, w_key, w_value, w_out, w_cquery, w_cout, w_gate, w_up, w_down,
                   self_k, self_v, cross_k, cross_v):
        def flat(cache):
            l, b, t, h, d = cache.shape
            return cache.transpose(0, 1, 3, 4, 2).reshape(l, b, h * d, t)

        def unflat(cache):
            l, b, _, t = cache.shape
            return cache.reshape(l, b, HEADS, 64, t).transpose(0, 1, 4, 2, 3)

        keys, vals = flat(self_k), flat(self_v)
        hidden, new = decode(
            h_first, h_second, start_pos, enc_lens, dec_bias.T, norm_self, norm_cross, norm_mlp,
            w_query, w_key, w_value, w_out, w_cquery, w_cout,
            w_gate.transpose(0, 2, 1), w_up.transpose(0, 2, 1), w_down,
            keys, vals, flat(cross_k), flat(cross_v))
        keys, vals = write_caches(start_pos, new, keys, vals)
        return hidden, unflat(keys), unflat(vals)

    row_spec = P(batch_axes, None)
    seq_spec = P(batch_axes)
    weight_spec = P(None, 'row', 'col')
    cache_spec = P(None, batch_axes)
    in_specs = (row_spec, row_spec, seq_spec, seq_spec, P(), P(), P(), P()) + (weight_spec,) * 9 + (cache_spec,) * 4
    out_specs = (P(None, batch_axes), cache_spec, cache_spec)
    return jax.shard_map(local_step, mesh=mesh, in_specs=in_specs, out_specs=out_specs, check_vma=False)
```

```python
import functools

import jax
import jax.numpy as jnp
from jax import lax
from jax.experimental import pallas as pl
from jax.experimental.pallas import tpu as pltpu
from jax.sharding import PartitionSpec as P

NORM_EPS = 1e-6
BUCKET_EDGES = (16, 19, 21, 24, 27, 31, 35, 40, 46, 52, 59, 67, 77, 87, 99, 113)
BUCKET_STARTS = tuple(range(16)) + BUCKET_EDGES
F32 = jnp.float32
BF16 = jnp.bfloat16
LAYERS = 2
SEQS = 2
TOK = 4
COLS = 4
ROWS = 4
PEERS = 16
D = 1024
HEADS = 16
T = 1024
E = 512
FB = 704
FS = 176
REPS = 3
NEG = float("-inf")

SCHEDULE = {
    0: (('a', 0),),
    1: (('in', 0, 0, (0, 2)),),
    2: (('b', 0), ('in', 0, 0, (1, 3))),
    3: (('c', 0), ('in', 0, 1, (0, 2))),
    4: (('d', 0), ('a', 1)),
    5: (('in', 0, 1, (1, 3)), ('e', 0), ('b', 1)),
    6: (('c', 1),),
    7: (('d', 1), ('a', 2)),
    8: (('e', 1), ('b', 2)),
    9: (('c', 2), ('in', 1, 0, (0, 2))),
    10: (('d', 2), ('in', 1, 0, (1, 3))),
    20: (('e', 2), ('in', 1, 1, (0, 2))),
    21: (('in', 1, 1, (1, 3)),),
}


def nt_dot(a, b):
    return lax.dot_general(a, b, (((1,), (1,)), ((), ())), preferred_element_type=F32)


def nn_dot(a, b):
    return jnp.dot(a, b, preferred_element_type=F32)


def body(h0_ref, h1_ref, pos_ref, len_ref, bias_ref, gs_ref, gc_ref, gm_ref,
         wq_hbm, wk_hbm, wv_hbm, wo_hbm, wcq_hbm, wco_hbm, wg_hbm, wu_hbm, wd_hbm,
         sk_hbm, sv_hbm, ck_hbm, cv_hbm,
         hid_ref, new_ref,
         sk, sv, ck, cv, self_bias, proj_w, gate_w, up_w, down_w,
         a_send, a_recv, p3_send, p3_recv, p1_send, p1_recv,
         n_send, n_recv, u_send, u_recv,
         rep, rep_send, rep_recv, cache_sem, weight_sem, mlp_send_sem, mlp_recv_sem, u_send_sem, u_recv_sem, send_sem, recv_sem):
    col = lax.axis_index('col')
    row = lax.axis_index('row')
    me = col * ROWS + row
    dp = lax.axis_index('dp')

    def peer_of(k):
        other = lax.rem(me + k, PEERS)
        return other, other // ROWS, lax.rem(other, ROWS)

    weight_copies = []
    for i, src in enumerate((wq_hbm, wk_hbm, wv_hbm, wo_hbm, wcq_hbm, wco_hbm)):
        cp = pltpu.make_async_copy(src, proj_w.at[i], weight_sem.at[i])
        cp.start()
        weight_copies.append(cp)
    cp = pltpu.make_async_copy(wd_hbm, down_w, weight_sem.at[6])
    cp.start()
    weight_copies.append(cp)
    cache_copies = []
    for l in range(LAYERS):
        for i, (src, dst) in enumerate(((sk_hbm, sk), (sv_hbm, sv), (ck_hbm, ck), (cv_hbm, cv))):
            cp = pltpu.make_async_copy(src.at[l], dst.at[l], cache_sem.at[l, i])
            cp.start()
            cache_copies.append(cp)

    barrier = pltpu.get_barrier_semaphore()
    for k in range(1, PEERS):
        _, c, r = peer_of(k)
        pl.semaphore_signal(barrier, inc=1, device_id={'col': c, 'row': r}, device_id_type=pl.DeviceIdType.MESH)
    pl.semaphore_signal(barrier, inc=1, device_id={'dp': 1 - dp}, device_id_type=pl.DeviceIdType.MESH)
    pl.semaphore_wait(barrier, PEERS)

    def exchange(send, recv, idx, by_row):
        def pick(r, other):
            return 0 if by_row is None else (r if by_row else other)

        for k in range(1, PEERS):
            other, c, r = peer_of(k)
            pltpu.make_async_remote_copy(
                src_ref=send.at[pick(r, other)], dst_ref=recv.at[me],
                send_sem=send_sem.at[idx], recv_sem=recv_sem.at[idx],
                device_id={'col': c, 'row': r}, device_id_type=pl.DeviceIdType.MESH).start()
        recv[me] = send[pick(row, me)]

    def arrive(recv, idx):
        part = recv.at[pl.ds(0, PEERS - 1)]
        pltpu.make_async_copy(part, part, recv_sem.at[idx]).wait()

    def left(recv, idx):
        part = recv.at[pl.ds(0, PEERS - 1)]
        pltpu.make_async_copy(part, part, send_sem.at[idx]).wait()

    def build_bias():
        jpos = lax.broadcasted_iota(jnp.int32, (HEADS, T), 1)
        for b in range(SEQS):
            p = pos_ref[b]
            for t in range(2):
                dist = p + t - jpos
                val = jnp.broadcast_to(bias_ref[:, 0:1], (HEADS, T))
                for n in range(1, 32):
                    val = jnp.where(dist >= BUCKET_STARTS[n], bias_ref[:, n:n + 1], val)
                self_bias[b, pl.ds(t * HEADS, HEADS), :] = jnp.where(jpos < p, val, NEG)

    r32 = lax.broadcasted_iota(jnp.int32, (32, 8), 0)
    c8 = lax.broadcasted_iota(jnp.int32, (32, 8), 1)
    db0 = jnp.concatenate([bias_ref[:, 0:1]] * 2, axis=0)
    db1 = jnp.concatenate([bias_ref[:, 1:2]] * 2, axis=0)
    new_bias = jnp.where(c8 == 0, jnp.where(r32 < HEADS, db0, db1),
                         jnp.where((c8 == 1) & (r32 >= HEADS), db0, NEG))
    head_of = (lax.broadcasted_iota(jnp.int32, (32, D), 1) // 64) == lax.rem(
        lax.broadcasted_iota(jnp.int32, (32, D), 0), HEADS)
    jcross = lax.broadcasted_iota(jnp.int32, (32, E), 1)

    def rms(x, gain):
        mean_sq = jnp.mean(x * x, axis=-1, keepdims=True)
        return x * lax.rsqrt(mean_sq + NORM_EPS) * gain.astype(F32)

    def put_act(vec, l, e):
        for r in range(ROWS):
            a_send[l, e, r] = vec[:, r * 256:(r + 1) * 256]

    def gather_act(recv):
        rows = jnp.concatenate([recv[s].astype(F32) for s in range(PEERS)], axis=0)
        return rows.astype(BF16)

    def spread_query(q4, b):
        q_first = jnp.broadcast_to(q4[b:b + 1, :], (HEADS, D))
        q_second = jnp.broadcast_to(q4[2 + b:3 + b, :], (HEADS, D))
        q = jnp.concatenate([q_first, q_second], axis=0)
        return jnp.where(head_of, q, 0.0).astype(BF16)

    def fold_heads(mixed):
        keep = jnp.where(head_of, mixed, 0.0)
        return (jnp.sum(keep[:HEADS], axis=0, keepdims=True), jnp.sum(keep[HEADS:], axis=0, keepdims=True))

    def join_tokens(pieces):
        return jnp.concatenate([pieces[0][0], pieces[1][0], pieces[0][1], pieces[1][1]], axis=0)

    def row_sum(get):
        return [(get(c * ROWS) + get(c * ROWS + 1)) + (get(c * ROWS + 2) + get(c * ROWS + 3)) for c in range(COLS)]

    def round_bf16(v):
        return v.astype(BF16).astype(F32)

    def project(vec, which, l, e, slot):
        put_act(vec, l, e)
        exchange(a_send.at[l, e], a_recv.at[l, e], l * 10 + slot, True)
        fill(l * 20 + slot)
        arrive(a_recv.at[l, e], l * 10 + slot)
        prod = nn_dot(gather_act(a_recv.at[l, e]), proj_w[which, l])
        for s in range(PEERS):
            p1_send[l, e - 1, s] = prod[s * TOK:(s + 1) * TOK, :]
        exchange(p1_send.at[l, e - 1], p1_recv.at[l, e - 1], l * 10 + slot + 1, False)
        fill(l * 20 + slot + 1)
        arrive(p1_recv.at[l, e - 1], l * 10 + slot + 1)
        sums = row_sum(lambda s: p1_recv[l, e - 1, s])
        return round_bf16(jnp.concatenate(sums, axis=1))

    def mlp_in(l, i, steps):
        src, dst = ((wg_hbm, gate_w), (wu_hbm, up_w))[i]
        for k in steps:
            r = lax.rem(row + k, ROWS)
            part = src.at[l, pl.ds(pl.multiple_of(r * FS, 16), FS), :]
            if k == 0:
                pltpu.make_async_copy(part, dst.at[l, row], mlp_recv_sem.at[l, i]).start()
            else:
                pltpu.make_async_remote_copy(
                    src_ref=part, dst_ref=dst.at[l, row], send_sem=mlp_send_sem.at[l, i],
                    recv_sem=mlp_recv_sem.at[l, i], device_id={'col': col, 'row': r},
                    device_id_type=pl.DeviceIdType.MESH).start()

    def send_u(l):
        for k in range(COLS):
            c = lax.rem(col + k, COLS)

            def away():
                pltpu.make_async_remote_copy(
                    src_ref=u_send.at[l], dst_ref=u_recv.at[l, row], send_sem=u_send_sem.at[l],
                    recv_sem=u_recv_sem.at[l], device_id={'col': c, 'row': col},
                    device_id_type=pl.DeviceIdType.MESH).start()

            if k == 0:
                pl.when(col != row)(away)

                @pl.when(col == row)
                def _():
                    pltpu.make_async_copy(u_send.at[l], u_recv.at[l, row], u_recv_sem.at[l]).start()
            else:
                away()

    own = (wo_hbm, wcq_hbm, wco_hbm)
    flip = lax.rem(row + 2, ROWS)
    twin = row + 1 - 2 * lax.rem(row, 2)
    up_col, down_col = lax.rem(col + 1, COLS), lax.rem(col + COLS - 1, COLS)

    def block_id(dz, other_y):
        return lax.rem(col + dz, COLS) * ROWS + (flip if other_y else row)

    def pass_on(m, step, src, j, device):
        pltpu.make_async_remote_copy(
            src_ref=src, dst_ref=rep.at[m, j], send_sem=rep_send.at[m], recv_sem=rep_recv.at[m, step],
            device_id=device, device_id_type=pl.DeviceIdType.MESH).start()

    def took(m, step, blocks):
        part = rep.at[m, pl.ds(0, blocks)]
        pltpu.make_async_copy(part, part, rep_recv.at[m, step]).wait()

    def rep_a(m):
        src = own[m].at[1]
        pltpu.make_async_copy(src, rep.at[m, me], rep_recv.at[m, 0]).start()
        for device in ({'row': flip}, {'col': up_col}, {'col': down_col}):
            pass_on(m, 0, src, me, device)

    def rep_b(m):
        took(m, 0, 4)
        ahead = block_id(1, False)
        beside = block_id(0, True)
        pass_on(m, 1, rep.at[m, beside], beside, {'col': up_col})
        pass_on(m, 1, rep.at[m, ahead], ahead, {'col': down_col})

        @pl.when(dp == 0)
        def _():
            pass_on(m, 1, rep.at[m, ahead], ahead, {'row': flip})

    def rep_c(m):
        @pl.when(dp == 0)
        def _():
            took(m, 1, 3)
            j = block_id(1, True)
            pass_on(m, 3, rep.at[m, j], j, {'dp': 1 - dp})

        @pl.when(dp == 1)
        def _():
            took(m, 1, 2)
            j = block_id(2, False)
            pass_on(m, 2, rep.at[m, j], j, {'row': flip})

    def rep_d(m):
        @pl.when(dp == 1)
        def _():
            took(m, 2, 1)
            j = block_id(2, True)
            pass_on(m, 3, rep.at[m, j], j, {'dp': 1 - dp})

    def rep_e(m):
        took(m, 3, 1)
        for dz in range(COLS):
            for other_y in (False, True):
                j = block_id(dz, other_y)
                pass_on(m, 4, rep.at[m, j], j, {'row': twin})

    def rep_left(m):
        part = rep.at[m, pl.ds(0, 15)]
        pltpu.make_async_copy(part, part, rep_send.at[m]).wait()

    def local_project(vec, m):
        took(m, 4, 8)
        sums = []
        for c in range(COLS):
            acc = nn_dot(vec[:, 0:256], rep[m, c * ROWS])
            for r in range(1, ROWS):
                acc = acc + nn_dot(vec[:, r * 256:(r + 1) * 256], rep[m, c * ROWS + r])
            sums.append(acc)
        return round_bf16(jnp.concatenate(sums, axis=1))

    work = SCHEDULE

    def fill(slot):
        for name, *what in work.get(slot, ()):
            {'in': mlp_in, 'a': rep_a, 'b': rep_b, 'c': rep_c, 'd': rep_d, 'e': rep_e}[name](*what)

    def mlp_arrive(l):
        for i, dst in enumerate((gate_w, up_w)):
            pltpu.make_async_copy(dst.at[l], dst.at[l], mlp_recv_sem.at[l, i]).wait()

    def mlp_left(l):
        for i, dst in enumerate((gate_w, up_w)):
            part = dst.at[l, pl.ds(0, ROWS - 1)]
            pltpu.make_async_copy(part, part, mlp_send_sem.at[l, i]).wait()
        part = u_recv.at[l, pl.ds(0, COLS - 1)]
        pltpu.make_async_copy(part, part, u_send_sem.at[l]).wait()

        @pl.when(col != row)
        def _():
            pltpu.make_async_copy(u_recv.at[l, 0], u_recv.at[l, 0], u_send_sem.at[l]).wait()

    def apply(vec, which, l, e, slot):
        return project(vec, which, l, e, slot) if l == 0 else local_project(vec, which - 3)

    x = jnp.concatenate([h0_ref[...].astype(F32), h1_ref[...].astype(F32)], axis=0)
    for l in range(LAYERS):
        base = l * 10
        n = rms(x, gs_ref[l:l + 1, :]).astype(BF16)
        put_act(n, l, 0)
        exchange(a_send.at[l, 0], a_recv.at[l, 0], base, True)
        fill(l * 20)
        if l == 0:
            build_bias()
            for cp in weight_copies:
                cp.wait()
        arrive(a_recv.at[l, 0], base)
        act = gather_act(a_recv.at[l, 0])
        for i in range(3):
            prod = nn_dot(act, proj_w[i, l])
            for s in range(PEERS):
                p3_send[l, s, :, i * 256:(i + 1) * 256] = prod[s * TOK:(s + 1) * TOK, :]
        exchange(p3_send.at[l], p3_recv.at[l], base + 1, False)
        fill(l * 20 + 1)
        arrive(p3_recv.at[l], base + 1)
        sums = row_sum(lambda s: p3_recv[l, s])
        q4, k4, v4 = (round_bf16(jnp.concatenate([sm[:, i * 256:(i + 1) * 256] for sm in sums], axis=1))
                      for i in range(3))
        new_ref[pl.ds(l * 8, TOK), :] = k4
        new_ref[pl.ds(l * 8 + TOK, TOK), :] = v4
        cache_copies[l * 4].wait()
        cache_copies[l * 4 + 1].wait()
        pieces = []
        for b in range(SEQS):
            qb = spread_query(q4, b)
            zeros = jnp.zeros((6, D), F32)
            kn = jnp.concatenate([k4[b:b + 1], k4[2 + b:3 + b], zeros], axis=0).astype(BF16)
            vn = jnp.concatenate([v4[b:b + 1], v4[2 + b:3 + b], zeros], axis=0).astype(BF16)
            old = nn_dot(qb, sk[l, b]) + self_bias[b]
            new = nt_dot(qb, kn) + new_bias
            top = jnp.maximum(jnp.max(old, axis=1, keepdims=True), jnp.max(new, axis=1, keepdims=True))
            e_old = jnp.exp(old - top)
            e_new = jnp.exp(new - top)
            total = jnp.sum(e_old, axis=1, keepdims=True) + jnp.sum(e_new, axis=1, keepdims=True)
            mixed = nt_dot((e_old / total).astype(BF16), sv[l, b]) + nn_dot((e_new / total).astype(BF16), vn)
            pieces.append(fold_heads(mixed))
        x = x + apply(join_tokens(pieces).astype(BF16), 3, l, 1, 2)

        n = rms(x, gc_ref[l:l + 1, :]).astype(BF16)
        q4 = apply(n, 4, l, 2, 4)
        cache_copies[l * 4 + 2].wait()
        cache_copies[l * 4 + 3].wait()
        pieces = []
        for b in range(SEQS):
            qb = spread_query(q4, b)
            sc = jnp.where(jcross < len_ref[b], nn_dot(qb, ck[l, b]), NEG)
            ex = jnp.exp(sc - jnp.max(sc, axis=1, keepdims=True))
            probs = (ex / jnp.sum(ex, axis=1, keepdims=True)).astype(BF16)
            pieces.append(fold_heads(nt_dot(probs, cv[l, b])))
        x = x + apply(join_tokens(pieces).astype(BF16), 5, l, 3, 6)

        n_send[l, 0] = rms(x, gm_ref[l:l + 1, :]).astype(BF16)
        exchange(n_send.at[l], n_recv.at[l], base + 8, None)
        fill(l * 20 + 8)
        mlp_arrive(l)
        arrive(n_recv.at[l], base + 8)
        act = gather_act(n_recv.at[l])
        gate = nt_dot(act[:, 0:256], gate_w[l, 0])
        up = nt_dot(act[:, 0:256], up_w[l, 0])
        for r in range(1, ROWS):
            gate = gate + nt_dot(act[:, r * 256:(r + 1) * 256], gate_w[l, r])
            up = up + nt_dot(act[:, r * 256:(r + 1) * 256], up_w[l, r])
        u_send[l] = (jax.nn.silu(round_bf16(gate)) * round_bf16(up)).astype(BF16)
        send_u(l)
        fill(l * 20 + 9)
        pltpu.make_async_copy(u_recv.at[l], u_recv.at[l], u_recv_sem.at[l]).wait()
        prod = nn_dot(u_recv[l, 0], down_w[l, 0:FS])
        for r in range(1, ROWS):
            prod = prod + nn_dot(u_recv[l, r], down_w[l, r * FS:(r + 1) * FS])
        for s in range(PEERS):
            p1_send[l, 3, s] = prod[s * TOK:(s + 1) * TOK, :]
        exchange(p1_send.at[l, 3], p1_recv.at[l, 3], l * 10 + 9, False)
        fill(l * 20 + 10)
        arrive(p1_recv.at[l, 3], l * 10 + 9)
        sums = row_sum(lambda s: p1_recv[l, 3, s])
        x = x + round_bf16(jnp.concatenate(sums, axis=1))

    hid_ref[0] = x[0:2].astype(BF16)
    hid_ref[1] = x[2:4].astype(BF16)
    for l in range(LAYERS):
        base = l * 10
        left(a_recv.at[l, 0], base)
        left(p3_recv.at[l], base + 1)
        for e in (1, 2, 3) if l == 0 else ():
            left(a_recv.at[l, e], base + 2 * e)
            left(p1_recv.at[l, e - 1], base + 2 * e + 1)
        left(n_recv.at[l], base + 8)
        left(p1_recv.at[l, 3], base + 9)
        mlp_left(l)
    for m in range(REPS):
        rep_left(m)


def write_body(pos_ref, new_ref, k_ref, v_ref, ko_ref, vo_ref, cols):
    i = pl.program_id(0)
    half = pl.program_id(1)

    @pl.when((i == 0) & (half == 0))
    def _():
        cols[...] = jnp.transpose(new_ref[...])

    b = lax.rem(i, SEQS)
    l = i // SEQS
    p = pos_ref[b]
    lanes = lax.broadcasted_iota(jnp.int32, (512, 128), 1)
    pick = lax.broadcasted_iota(jnp.int32, (512, 16), 1)
    mine = cols[pl.ds(pl.multiple_of(half * 512, 512), 512), :]
    for kv, (src, dst) in enumerate(((k_ref, ko_ref), (v_ref, vo_ref))):
        dst[...] = src[...]
        at = l * 8 + kv * TOK + b
        first = jnp.sum(jnp.where(pick == at, mine, 0.0), axis=1, keepdims=True)
        second = jnp.sum(jnp.where(pick == at + 2, mine, 0.0), axis=1, keepdims=True)
        for q in range(2):
            start = pl.multiple_of(((p + q) // 128) * 128, 128)
            old = src[0, 0, :, pl.ds(start, 128)].astype(F32)
            fresh = jnp.where(lanes + start == p, first, jnp.where(lanes + start == p + 1, second, old))
            dst[0, 0, :, pl.ds(start, 128)] = fresh.astype(BF16)


def write_caches(pos, new, k, v):
    block = pl.BlockSpec((1, 1, 512, T), lambda i, j: (i // SEQS, i % SEQS, j, 0))
    return pl.pallas_call(
        write_body,
        grid=(LAYERS * SEQS, 2),
        out_shape=(jax.ShapeDtypeStruct(k.shape, BF16),) * 2,
        in_specs=[pl.BlockSpec(memory_space=pltpu.SMEM), pl.BlockSpec((16, D), lambda i, j: (0, 0)), block, block],
        out_specs=(block, block),
        scratch_shapes=[pltpu.VMEM((D, 16), F32)],
        compiler_params=pltpu.CompilerParams(vmem_limit_bytes=14 * 1024 * 1024),
        cost_estimate=pl.CostEstimate(flops=1000000, bytes_accessed=32 << 20, transcendentals=0),
    )(pos, new, k, v)


def decode(*args):
    vmem = pl.BlockSpec(memory_space=pltpu.VMEM)
    smem = pl.BlockSpec(memory_space=pltpu.SMEM)
    hbm = pl.BlockSpec(memory_space=pltpu.HBM)
    args = tuple(pltpu.with_memory_space_constraint(a, pltpu.HBM) for a in args)
    return pl.pallas_call(
        body,
        out_shape=(jax.ShapeDtypeStruct((2, SEQS, D), BF16),
                   jax.ShapeDtypeStruct((16, D), F32)),
        in_specs=[vmem, vmem, smem, smem] + [vmem] * 4 + [hbm] * 13,
        out_specs=(vmem,) * 2,
        scratch_shapes=[
            pltpu.VMEM((LAYERS, SEQS, D, T), BF16),
            pltpu.VMEM((LAYERS, SEQS, D, T), BF16),
            pltpu.VMEM((LAYERS, SEQS, D, E), BF16),
            pltpu.VMEM((LAYERS, SEQS, D, E), BF16),
            pltpu.VMEM((SEQS, 32, T), F32),
            pltpu.VMEM((6, LAYERS, 256, 256), BF16),
            pltpu.VMEM((LAYERS, ROWS, FS, 256), BF16),
            pltpu.VMEM((LAYERS, ROWS, FS, 256), BF16),
            pltpu.VMEM((LAYERS, FB, 256), BF16),
            pltpu.VMEM((LAYERS, 4, ROWS, TOK, 256), BF16),
            pltpu.VMEM((LAYERS, 4, PEERS, TOK, 256), BF16),
            pltpu.VMEM((LAYERS, PEERS, TOK, 768), F32),
            pltpu.VMEM((LAYERS, PEERS, TOK, 768), F32),
            pltpu.VMEM((LAYERS, 4, PEERS, TOK, 256), F32),
            pltpu.VMEM((LAYERS, 4, PEERS, TOK, 256), F32),
            pltpu.VMEM((LAYERS, 1, TOK, D), BF16),
            pltpu.VMEM((LAYERS, PEERS, TOK, D), BF16),
            pltpu.VMEM((LAYERS, PEERS * TOK, FS), BF16),
            pltpu.VMEM((LAYERS, ROWS, PEERS * TOK, FS), BF16),
            pltpu.VMEM((REPS, PEERS, 256, 256), BF16),
            pltpu.SemaphoreType.DMA((REPS,)),
            pltpu.SemaphoreType.DMA((REPS, 5)),
            pltpu.SemaphoreType.DMA((LAYERS, 4)),
            pltpu.SemaphoreType.DMA((7,)),
            pltpu.SemaphoreType.DMA((LAYERS, 2)),
            pltpu.SemaphoreType.DMA((LAYERS, 2)),
            pltpu.SemaphoreType.DMA((LAYERS,)),
            pltpu.SemaphoreType.DMA((LAYERS,)),
            pltpu.SemaphoreType.DMA((LAYERS * 10,)),
            pltpu.SemaphoreType.DMA((LAYERS * 10,)),
        ],
        compiler_params=pltpu.CompilerParams(collective_id=0, has_side_effects=True,
                                             vmem_limit_bytes=44 * 1024 * 1024),
        cost_estimate=pl.CostEstimate(flops=400000000, bytes_accessed=32 << 20, transcendentals=0),
    )(*args)


def solution(mesh):
    batch_axes = ('dp', 'col', 'row')

    def local_step(h_first, h_second, start_pos, enc_lens, dec_bias, norm_self, norm_cross, norm_mlp,
                   w_query, w_key, w_value, w_out, w_cquery, w_cout, w_gate, w_up, w_down,
                   self_k, self_v, cross_k, cross_v):
        def flat(cache):
            l, b, t, h, d = cache.shape
            return cache.transpose(0, 1, 3, 4, 2).reshape(l, b, h * d, t)

        def unflat(cache):
            l, b, _, t = cache.shape
            return cache.reshape(l, b, HEADS, 64, t).transpose(0, 1, 4, 2, 3)

        keys, vals = flat(self_k), flat(self_v)
        hidden, new = decode(
            h_first, h_second, start_pos, enc_lens, dec_bias.T, norm_self, norm_cross, norm_mlp,
            w_query, w_key, w_value, w_out, w_cquery, w_cout,
            w_gate.transpose(0, 2, 1), w_up.transpose(0, 2, 1), w_down,
            keys, vals, flat(cross_k), flat(cross_v))
        keys, vals = write_caches(start_pos, new, keys, vals)
        return hidden, unflat(keys), unflat(vals)

    row_spec = P(batch_axes, None)
    seq_spec = P(batch_axes)
    weight_spec = P(None, 'row', 'col')
    cache_spec = P(None, batch_axes)
    in_specs = (row_spec, row_spec, seq_spec, seq_spec, P(), P(), P(), P()) + (weight_spec,) * 9 + (cache_spec,) * 4
    out_specs = (P(None, batch_axes), cache_spec, cache_spec)
    return jax.shard_map(local_step, mesh=mesh, in_specs=in_specs, out_specs=out_specs, check_vma=False)
```

```python
import functools

import jax
import jax.numpy as jnp
from jax import lax
from jax.experimental import pallas as pl
from jax.experimental.pallas import tpu as pltpu
from jax.sharding import PartitionSpec as P

NORM_EPS = 1e-6
BUCKET_EDGES = (16, 19, 21, 24, 27, 31, 35, 40, 46, 52, 59, 67, 77, 87, 99, 113)
BUCKET_STARTS = tuple(range(16)) + BUCKET_EDGES
F32 = jnp.float32
BF16 = jnp.bfloat16
LAYERS = 2
SEQS = 2
TOK = 4
COLS = 4
ROWS = 4
PEERS = 16
D = 1024
HEADS = 16
T = 1024
E = 512
FB = 704
FS = 176
REPS = 3
NEG = float("-inf")

SCHEDULE = {
    0: (('z', 0, 1), ('y', 0, 0)),
    1: (('in', 0, 0, (0, 2)),),
    2: (('z', 0, 2), ('y', 0, 1), ('in', 0, 0, (1, 3))),
    3: (('z', 0, 3), ('in', 0, 1, (0, 2))),
    4: (('y', 0, 2), ('z', 1, 1), ('y', 1, 0)),
    5: (('y', 0, 3), ('z', 1, 2), ('in', 0, 1, (1, 3))),
    6: (('z', 1, 3), ('y', 1, 1), ('x', 0)),
    7: (('y', 1, 2), ('z', 2, 1), ('y', 2, 0)),
    8: (('e', 0), ('y', 1, 3), ('z', 2, 3)),
    9: (('y', 2, 1), ('x', 1), ('in', 1, 0, (0, 2))),
    10: (('z', 2, 2), ('y', 2, 3), ('in', 1, 0, (1, 3))),
    20: (('e', 1), ('y', 2, 2), ('in', 1, 1, (0, 2))),
    21: (('x', 2), ('in', 1, 1, (1, 3))),
    50: (('e', 2),),
}


def nt_dot(a, b):
    return lax.dot_general(a, b, (((1,), (1,)), ((), ())), preferred_element_type=F32)


def nn_dot(a, b):
    return jnp.dot(a, b, preferred_element_type=F32)


def body(h0_ref, h1_ref, pos_ref, len_ref, bias_ref, gs_ref, gc_ref, gm_ref,
         wq_hbm, wk_hbm, wv_hbm, wo_hbm, wcq_hbm, wco_hbm, wg_hbm, wu_hbm, wd_hbm,
         sk_hbm, sv_hbm, ck_hbm, cv_hbm,
         hid_ref, new_ref,
         sk, sv, ck, cv, self_bias, proj_w, gate_w, up_w, down_w,
         a_send, a_recv, p3_send, p3_recv, p1_send, p1_recv,
         n_send, n_recv, u_send, u_recv,
         rep, rep_send, rep_recv, cache_sem, weight_sem, mlp_send_sem, mlp_recv_sem, u_send_sem, u_recv_sem, send_sem, recv_sem):
    col = lax.axis_index('col')
    row = lax.axis_index('row')
    me = col * ROWS + row
    dp = lax.axis_index('dp')

    def peer_of(k):
        other = lax.rem(me + k, PEERS)
        return other, other // ROWS, lax.rem(other, ROWS)

    weight_copies = []
    for i, src in enumerate((wq_hbm, wk_hbm, wv_hbm, wo_hbm, wcq_hbm, wco_hbm)):
        cp = pltpu.make_async_copy(src, proj_w.at[i], weight_sem.at[i])
        cp.start()
        weight_copies.append(cp)
    cp = pltpu.make_async_copy(wd_hbm, down_w, weight_sem.at[6])
    cp.start()
    weight_copies.append(cp)
    cache_copies = []
    for l in range(LAYERS):
        for i, (src, dst) in enumerate(((sk_hbm, sk), (sv_hbm, sv), (ck_hbm, ck), (cv_hbm, cv))):
            cp = pltpu.make_async_copy(src.at[l], dst.at[l], cache_sem.at[l, i])
            cp.start()
            cache_copies.append(cp)

    barrier = pltpu.get_barrier_semaphore()
    for k in range(1, PEERS):
        _, c, r = peer_of(k)
        pl.semaphore_signal(barrier, inc=1, device_id={'col': c, 'row': r}, device_id_type=pl.DeviceIdType.MESH)
    pl.semaphore_signal(barrier, inc=1, device_id={'dp': 1 - dp}, device_id_type=pl.DeviceIdType.MESH)
    pl.semaphore_wait(barrier, PEERS)

    def exchange(send, recv, idx, by_row):
        def pick(r, other):
            return 0 if by_row is None else (r if by_row else other)

        for k in range(1, PEERS):
            other, c, r = peer_of(k)
            pltpu.make_async_remote_copy(
                src_ref=send.at[pick(r, other)], dst_ref=recv.at[me],
                send_sem=send_sem.at[idx], recv_sem=recv_sem.at[idx],
                device_id={'col': c, 'row': r}, device_id_type=pl.DeviceIdType.MESH).start()
        recv[me] = send[pick(row, me)]

    def arrive(recv, idx):
        part = recv.at[pl.ds(0, PEERS - 1)]
        pltpu.make_async_copy(part, part, recv_sem.at[idx]).wait()

    def left(recv, idx):
        part = recv.at[pl.ds(0, PEERS - 1)]
        pltpu.make_async_copy(part, part, send_sem.at[idx]).wait()

    def build_bias():
        jpos = lax.broadcasted_iota(jnp.int32, (HEADS, T), 1)
        for b in range(SEQS):
            p = pos_ref[b]
            for t in range(2):
                dist = p + t - jpos
                val = jnp.broadcast_to(bias_ref[:, 0:1], (HEADS, T))
                for n in range(1, 32):
                    val = jnp.where(dist >= BUCKET_STARTS[n], bias_ref[:, n:n + 1], val)
                self_bias[b, pl.ds(t * HEADS, HEADS), :] = jnp.where(jpos < p, val, NEG)

    r32 = lax.broadcasted_iota(jnp.int32, (32, 8), 0)
    c8 = lax.broadcasted_iota(jnp.int32, (32, 8), 1)
    db0 = jnp.concatenate([bias_ref[:, 0:1]] * 2, axis=0)
    db1 = jnp.concatenate([bias_ref[:, 1:2]] * 2, axis=0)
    new_bias = jnp.where(c8 == 0, jnp.where(r32 < HEADS, db0, db1),
                         jnp.where((c8 == 1) & (r32 >= HEADS), db0, NEG))
    head_of = (lax.broadcasted_iota(jnp.int32, (32, D), 1) // 64) == lax.rem(
        lax.broadcasted_iota(jnp.int32, (32, D), 0), HEADS)
    jcross = lax.broadcasted_iota(jnp.int32, (32, E), 1)

    def rms(x, gain):
        mean_sq = jnp.mean(x * x, axis=-1, keepdims=True)
        return x * lax.rsqrt(mean_sq + NORM_EPS) * gain.astype(F32)

    def put_act(vec, l, e):
        for r in range(ROWS):
            a_send[l, e, r] = vec[:, r * 256:(r + 1) * 256]

    def gather_act(recv):
        rows = jnp.concatenate([recv[s].astype(F32) for s in range(PEERS)], axis=0)
        return rows.astype(BF16)

    def spread_query(q4, b):
        q_first = jnp.broadcast_to(q4[b:b + 1, :], (HEADS, D))
        q_second = jnp.broadcast_to(q4[2 + b:3 + b, :], (HEADS, D))
        q = jnp.concatenate([q_first, q_second], axis=0)
        return jnp.where(head_of, q, 0.0).astype(BF16)

    def fold_heads(mixed):
        keep = jnp.where(head_of, mixed, 0.0)
        return (jnp.sum(keep[:HEADS], axis=0, keepdims=True), jnp.sum(keep[HEADS:], axis=0, keepdims=True))

    def join_tokens(pieces):
        return jnp.concatenate([pieces[0][0], pieces[1][0], pieces[0][1], pieces[1][1]], axis=0)

    def row_sum(get):
        return [(get(c * ROWS) + get(c * ROWS + 1)) + (get(c * ROWS + 2) + get(c * ROWS + 3)) for c in range(COLS)]

    def round_bf16(v):
        return v.astype(BF16).astype(F32)

    def project(vec, which, l, e, slot):
        put_act(vec, l, e)
        exchange(a_send.at[l, e], a_recv.at[l, e], l * 10 + slot, True)
        fill(l * 20 + slot)
        arrive(a_recv.at[l, e], l * 10 + slot)
        prod = nn_dot(gather_act(a_recv.at[l, e]), proj_w[which, l])
        for s in range(PEERS):
            p1_send[l, e - 1, s] = prod[s * TOK:(s + 1) * TOK, :]
        exchange(p1_send.at[l, e - 1], p1_recv.at[l, e - 1], l * 10 + slot + 1, False)
        fill(l * 20 + slot + 1)
        arrive(p1_recv.at[l, e - 1], l * 10 + slot + 1)
        sums = row_sum(lambda s: p1_recv[l, e - 1, s])
        return round_bf16(jnp.concatenate(sums, axis=1))

    def mlp_in(l, i, steps):
        src, dst = ((wg_hbm, gate_w), (wu_hbm, up_w))[i]
        for k in steps:
            r = lax.rem(row + k, ROWS)
            part = src.at[l, pl.ds(pl.multiple_of(r * FS, 16), FS), :]
            if k == 0:
                pltpu.make_async_copy(part, dst.at[l, row], mlp_recv_sem.at[l, i]).start()
            else:
                pltpu.make_async_remote_copy(
                    src_ref=part, dst_ref=dst.at[l, row], send_sem=mlp_send_sem.at[l, i],
                    recv_sem=mlp_recv_sem.at[l, i], device_id={'col': col, 'row': r},
                    device_id_type=pl.DeviceIdType.MESH).start()

    def send_u(l):
        for k in range(COLS):
            c = lax.rem(col + k, COLS)

            def away():
                pltpu.make_async_remote_copy(
                    src_ref=u_send.at[l], dst_ref=u_recv.at[l, row], send_sem=u_send_sem.at[l],
                    recv_sem=u_recv_sem.at[l], device_id={'col': c, 'row': col},
                    device_id_type=pl.DeviceIdType.MESH).start()

            if k == 0:
                pl.when(col != row)(away)

                @pl.when(col == row)
                def _():
                    pltpu.make_async_copy(u_send.at[l], u_recv.at[l, row], u_recv_sem.at[l]).start()
            else:
                away()

    own = (wo_hbm, wcq_hbm, wco_hbm)
    flip = lax.rem(row + 2, ROWS)
    twin = row + 1 - 2 * lax.rem(row, 2)
    first_row = pl.multiple_of(dp * 128, 128)

    def half(m, j):
        return rep.at[m, j, pl.ds(first_row, 128), :]

    def pass_on(m, step, src, dst, device):
        pltpu.make_async_remote_copy(
            src_ref=src, dst_ref=dst, send_sem=rep_send.at[m], recv_sem=rep_recv.at[m, step],
            device_id=device, device_id_type=pl.DeviceIdType.MESH).start()

    def took(m, step, blocks):
        part = rep.at[m, pl.ds(0, blocks)]
        pltpu.make_async_copy(part, part, rep_recv.at[m, step]).wait()

    def took_halves(m, step, halves):
        part = rep.at[m, pl.ds(0, halves), pl.ds(0, 128), :]
        pltpu.make_async_copy(part, part, rep_recv.at[m, step]).wait()

    def rep_z(m, k):
        if k == 1:
            pltpu.make_async_copy(own[m].at[1], rep.at[m, me], rep_recv.at[m, 6]).start()
        pass_on(m, k - 1, own[m].at[1, pl.ds(first_row, 128), :], half(m, me), {'col': lax.rem(col + k, COLS)})

    def rep_y(m, k):
        j = lax.rem(col + COLS - k, COLS) * ROWS + row
        if k == 0:
            pass_on(m, 3, own[m].at[1, pl.ds(first_row, 128), :], half(m, j), {'row': flip})
        else:
            took_halves(m, k - 1, 1)
            pass_on(m, 3, half(m, j), half(m, j), {'row': flip})
            pass_on(m, 4, half(m, j), half(m, j), {'dp': 1 - dp})

    def rep_x(m):
        took_halves(m, 3, 4)
        for c in range(COLS):
            j = c * ROWS + flip
            pass_on(m, 4, half(m, j), half(m, j), {'dp': 1 - dp})

    def rep_e(m):
        took_halves(m, 4, 7)
        took(m, 6, 1)
        for c in range(COLS):
            for r in (row, flip):
                j = c * ROWS + r
                pass_on(m, 5, rep.at[m, j], rep.at[m, j], {'row': twin})

    def rep_left(m):
        part = rep.at[m, pl.ds(0, 15)]
        pltpu.make_async_copy(part, part, rep_send.at[m]).wait()

    def local_project(vec, m):
        took(m, 5, 8)
        sums = []
        for c in range(COLS):
            acc = nn_dot(vec[:, 0:256], rep[m, c * ROWS])
            for r in range(1, ROWS):
                acc = acc + nn_dot(vec[:, r * 256:(r + 1) * 256], rep[m, c * ROWS + r])
            sums.append(acc)
        return round_bf16(jnp.concatenate(sums, axis=1))

    work = SCHEDULE

    def fill(slot):
        for name, *what in work.get(slot, ()):
            {'in': mlp_in, 'z': rep_z, 'y': rep_y, 'x': rep_x, 'e': rep_e}[name](*what)

    def mlp_arrive(l):
        for i, dst in enumerate((gate_w, up_w)):
            pltpu.make_async_copy(dst.at[l], dst.at[l], mlp_recv_sem.at[l, i]).wait()

    def mlp_left(l):
        for i, dst in enumerate((gate_w, up_w)):
            part = dst.at[l, pl.ds(0, ROWS - 1)]
            pltpu.make_async_copy(part, part, mlp_send_sem.at[l, i]).wait()
        part = u_recv.at[l, pl.ds(0, COLS - 1)]
        pltpu.make_async_copy(part, part, u_send_sem.at[l]).wait()

        @pl.when(col != row)
        def _():
            pltpu.make_async_copy(u_recv.at[l, 0], u_recv.at[l, 0], u_send_sem.at[l]).wait()

    def apply(vec, which, l, e, slot):
        return project(vec, which, l, e, slot) if l == 0 else local_project(vec, which - 3)

    x = jnp.concatenate([h0_ref[...].astype(F32), h1_ref[...].astype(F32)], axis=0)
    for l in range(LAYERS):
        base = l * 10
        n = rms(x, gs_ref[l:l + 1, :]).astype(BF16)
        put_act(n, l, 0)
        exchange(a_send.at[l, 0], a_recv.at[l, 0], base, True)
        fill(l * 20)
        if l == 0:
            build_bias()
            for cp in weight_copies:
                cp.wait()
        arrive(a_recv.at[l, 0], base)
        act = gather_act(a_recv.at[l, 0])
        for i in range(3):
            prod = nn_dot(act, proj_w[i, l])
            for s in range(PEERS):
                p3_send[l, s, :, i * 256:(i + 1) * 256] = prod[s * TOK:(s + 1) * TOK, :]
        exchange(p3_send.at[l], p3_recv.at[l], base + 1, False)
        fill(l * 20 + 1)
        arrive(p3_recv.at[l], base + 1)
        sums = row_sum(lambda s: p3_recv[l, s])
        q4, k4, v4 = (round_bf16(jnp.concatenate([sm[:, i * 256:(i + 1) * 256] for sm in sums], axis=1))
                      for i in range(3))
        new_ref[pl.ds(l * 8, TOK), :] = k4
        new_ref[pl.ds(l * 8 + TOK, TOK), :] = v4
        cache_copies[l * 4].wait()
        cache_copies[l * 4 + 1].wait()
        pieces = []
        for b in range(SEQS):
            qb = spread_query(q4, b)
            zeros = jnp.zeros((6, D), F32)
            kn = jnp.concatenate([k4[b:b + 1], k4[2 + b:3 + b], zeros], axis=0).astype(BF16)
            vn = jnp.concatenate([v4[b:b + 1], v4[2 + b:3 + b], zeros], axis=0).astype(BF16)
            old = nn_dot(qb, sk[l, b]) + self_bias[b]
            new = nt_dot(qb, kn) + new_bias
            top = jnp.maximum(jnp.max(old, axis=1, keepdims=True), jnp.max(new, axis=1, keepdims=True))
            e_old = jnp.exp(old - top)
            e_new = jnp.exp(new - top)
            total = jnp.sum(e_old, axis=1, keepdims=True) + jnp.sum(e_new, axis=1, keepdims=True)
            mixed = nt_dot((e_old / total).astype(BF16), sv[l, b]) + nn_dot((e_new / total).astype(BF16), vn)
            pieces.append(fold_heads(mixed))
        x = x + apply(join_tokens(pieces).astype(BF16), 3, l, 1, 2)

        n = rms(x, gc_ref[l:l + 1, :]).astype(BF16)
        q4 = apply(n, 4, l, 2, 4)
        fill(l * 20 + 30)
        cache_copies[l * 4 + 2].wait()
        cache_copies[l * 4 + 3].wait()
        pieces = []
        for b in range(SEQS):
            qb = spread_query(q4, b)
            sc = jnp.where(jcross < len_ref[b], nn_dot(qb, ck[l, b]), NEG)
            ex = jnp.exp(sc - jnp.max(sc, axis=1, keepdims=True))
            probs = (ex / jnp.sum(ex, axis=1, keepdims=True)).astype(BF16)
            pieces.append(fold_heads(nt_dot(probs, cv[l, b])))
        x = x + apply(join_tokens(pieces).astype(BF16), 5, l, 3, 6)

        n_send[l, 0] = rms(x, gm_ref[l:l + 1, :]).astype(BF16)
        exchange(n_send.at[l], n_recv.at[l], base + 8, None)
        fill(l * 20 + 8)
        mlp_arrive(l)
        arrive(n_recv.at[l], base + 8)
        act = gather_act(n_recv.at[l])
        gate = nt_dot(act[:, 0:256], gate_w[l, 0])
        up = nt_dot(act[:, 0:256], up_w[l, 0])
        for r in range(1, ROWS):
            gate = gate + nt_dot(act[:, r * 256:(r + 1) * 256], gate_w[l, r])
            up = up + nt_dot(act[:, r * 256:(r + 1) * 256], up_w[l, r])
        u_send[l] = (jax.nn.silu(round_bf16(gate)) * round_bf16(up)).astype(BF16)
        send_u(l)
        fill(l * 20 + 9)
        pltpu.make_async_copy(u_recv.at[l], u_recv.at[l], u_recv_sem.at[l]).wait()
        prod = nn_dot(u_recv[l, 0], down_w[l, 0:FS])
        for r in range(1, ROWS):
            prod = prod + nn_dot(u_recv[l, r], down_w[l, r * FS:(r + 1) * FS])
        for s in range(PEERS):
            p1_send[l, 3, s] = prod[s * TOK:(s + 1) * TOK, :]
        exchange(p1_send.at[l, 3], p1_recv.at[l, 3], l * 10 + 9, False)
        fill(l * 20 + 10)
        arrive(p1_recv.at[l, 3], l * 10 + 9)
        sums = row_sum(lambda s: p1_recv[l, 3, s])
        x = x + round_bf16(jnp.concatenate(sums, axis=1))

    hid_ref[0] = x[0:2].astype(BF16)
    hid_ref[1] = x[2:4].astype(BF16)
    for l in range(LAYERS):
        base = l * 10
        left(a_recv.at[l, 0], base)
        left(p3_recv.at[l], base + 1)
        for e in (1, 2, 3) if l == 0 else ():
            left(a_recv.at[l, e], base + 2 * e)
            left(p1_recv.at[l, e - 1], base + 2 * e + 1)
        left(n_recv.at[l], base + 8)
        left(p1_recv.at[l, 3], base + 9)
        mlp_left(l)
    for m in range(REPS):
        rep_left(m)


def write_body(pos_ref, new_ref, k_ref, v_ref, ko_ref, vo_ref, cols, patch, sem):
    lanes = lax.broadcasted_iota(jnp.int32, (D, 128), 1)
    blocks = [(l, b, kv) for l in range(LAYERS) for b in range(SEQS) for kv in range(2)]

    def refs(kv):
        return (k_ref, ko_ref) if kv == 0 else (v_ref, vo_ref)

    def tiles(l, b, kv, put):
        first, second = pos_ref[b] // 128, (pos_ref[b] + 1) // 128
        src, dst = refs(kv)
        for i in range(T // 128):
            out = dst.at[l, b, :, pl.ds(i * 128, 128)]
            put(i, first, second, src.at[l, b, :, pl.ds(i * 128, 128)], out)

    for l, b, kv in blocks:
        def plain(i, first, second, src, out):
            @pl.when((first != i) & (second != i))
            def _():
                pltpu.make_async_copy(src, out, sem.at[l, b, kv]).start()

        tiles(l, b, kv, plain)

    cols[...] = jnp.transpose(new_ref[...])
    for l, b, kv in blocks:
        p = pos_ref[b]
        at = l * 8 + kv * TOK + b
        src, _ = refs(kv)
        for q in range(2):
            start = pl.multiple_of(((p + q) // 128) * 128, 128)
            old = src[l, b, :, pl.ds(start, 128)].astype(F32)
            fresh = jnp.where(lanes + start == p, cols[:, at:at + 1],
                              jnp.where(lanes + start == p + 1, cols[:, at + 2:at + 3], old))
            patch[l, b, kv, q] = fresh.astype(BF16)

        def changed(i, first, second, src, out):
            @pl.when(first == i)
            def _():
                pltpu.make_async_copy(patch.at[l, b, kv, 0], out, sem.at[l, b, kv]).start()

            @pl.when((second == i) & (first != i))
            def _():
                pltpu.make_async_copy(patch.at[l, b, kv, 1], out, sem.at[l, b, kv]).start()

        tiles(l, b, kv, changed)
    for l, b, kv in blocks:
        src, dst = refs(kv)
        pltpu.make_async_copy(src.at[l, b], dst.at[l, b], sem.at[l, b, kv]).wait()


def write_caches(pos, new, k, v):
    vmem = pl.BlockSpec(memory_space=pltpu.VMEM)
    return pl.pallas_call(
        write_body,
        out_shape=(jax.ShapeDtypeStruct(k.shape, BF16),) * 2,
        in_specs=[pl.BlockSpec(memory_space=pltpu.SMEM), vmem, vmem, vmem],
        out_specs=(pl.BlockSpec(memory_space=pltpu.HBM),) * 2,
        scratch_shapes=[pltpu.VMEM((D, 16), F32), pltpu.VMEM((LAYERS, SEQS, 2, 2, D, 128), BF16),
                        pltpu.SemaphoreType.DMA((LAYERS, SEQS, 2))],
        compiler_params=pltpu.CompilerParams(vmem_limit_bytes=28 * 1024 * 1024),
        cost_estimate=pl.CostEstimate(flops=1000000, bytes_accessed=32 << 20, transcendentals=0),
    )(pos, new, k, v)


def decode(*args):
    vmem = pl.BlockSpec(memory_space=pltpu.VMEM)
    smem = pl.BlockSpec(memory_space=pltpu.SMEM)
    hbm = pl.BlockSpec(memory_space=pltpu.HBM)
    args = tuple(pltpu.with_memory_space_constraint(a, pltpu.HBM) for a in args)
    return pl.pallas_call(
        body,
        out_shape=(jax.ShapeDtypeStruct((2, SEQS, D), BF16),
                   jax.ShapeDtypeStruct((16, D), F32)),
        in_specs=[vmem, vmem, smem, smem] + [vmem] * 4 + [hbm] * 13,
        out_specs=(vmem,) * 2,
        scratch_shapes=[
            pltpu.VMEM((LAYERS, SEQS, D, T), BF16),
            pltpu.VMEM((LAYERS, SEQS, D, T), BF16),
            pltpu.VMEM((LAYERS, SEQS, D, E), BF16),
            pltpu.VMEM((LAYERS, SEQS, D, E), BF16),
            pltpu.VMEM((SEQS, 32, T), F32),
            pltpu.VMEM((6, LAYERS, 256, 256), BF16),
            pltpu.VMEM((LAYERS, ROWS, FS, 256), BF16),
            pltpu.VMEM((LAYERS, ROWS, FS, 256), BF16),
            pltpu.VMEM((LAYERS, FB, 256), BF16),
            pltpu.VMEM((LAYERS, 4, ROWS, TOK, 256), BF16),
            pltpu.VMEM((LAYERS, 4, PEERS, TOK, 256), BF16),
            pltpu.VMEM((LAYERS, PEERS, TOK, 768), F32),
            pltpu.VMEM((LAYERS, PEERS, TOK, 768), F32),
            pltpu.VMEM((LAYERS, 4, PEERS, TOK, 256), F32),
            pltpu.VMEM((LAYERS, 4, PEERS, TOK, 256), F32),
            pltpu.VMEM((LAYERS, 1, TOK, D), BF16),
            pltpu.VMEM((LAYERS, PEERS, TOK, D), BF16),
            pltpu.VMEM((LAYERS, PEERS * TOK, FS), BF16),
            pltpu.VMEM((LAYERS, ROWS, PEERS * TOK, FS), BF16),
            pltpu.VMEM((REPS, PEERS, 256, 256), BF16),
            pltpu.SemaphoreType.DMA((REPS,)),
            pltpu.SemaphoreType.DMA((REPS, 7)),
            pltpu.SemaphoreType.DMA((LAYERS, 4)),
            pltpu.SemaphoreType.DMA((7,)),
            pltpu.SemaphoreType.DMA((LAYERS, 2)),
            pltpu.SemaphoreType.DMA((LAYERS, 2)),
            pltpu.SemaphoreType.DMA((LAYERS,)),
            pltpu.SemaphoreType.DMA((LAYERS,)),
            pltpu.SemaphoreType.DMA((LAYERS * 10,)),
            pltpu.SemaphoreType.DMA((LAYERS * 10,)),
        ],
        compiler_params=pltpu.CompilerParams(collective_id=0, has_side_effects=True,
                                             vmem_limit_bytes=44 * 1024 * 1024),
        cost_estimate=pl.CostEstimate(flops=400000000, bytes_accessed=32 << 20, transcendentals=0),
    )(*args)


def solution(mesh):
    batch_axes = ('dp', 'col', 'row')

    def local_step(h_first, h_second, start_pos, enc_lens, dec_bias, norm_self, norm_cross, norm_mlp,
                   w_query, w_key, w_value, w_out, w_cquery, w_cout, w_gate, w_up, w_down,
                   self_k, self_v, cross_k, cross_v):
        def flat(cache):
            l, b, t, h, d = cache.shape
            return cache.transpose(0, 1, 3, 4, 2).reshape(l, b, h * d, t)

        def unflat(cache):
            l, b, _, t = cache.shape
            return cache.reshape(l, b, HEADS, 64, t).transpose(0, 1, 4, 2, 3)

        keys, vals = flat(self_k), flat(self_v)
        hidden, new = decode(
            h_first, h_second, start_pos, enc_lens, dec_bias.T, norm_self, norm_cross, norm_mlp,
            w_query, w_key, w_value, w_out, w_cquery, w_cout,
            w_gate.transpose(0, 2, 1), w_up.transpose(0, 2, 1), w_down,
            keys, vals, flat(cross_k), flat(cross_v))
        keys, vals = write_caches(start_pos, new, keys, vals)
        return hidden, unflat(keys), unflat(vals)

    row_spec = P(batch_axes, None)
    seq_spec = P(batch_axes)
    weight_spec = P(None, 'row', 'col')
    cache_spec = P(None, batch_axes)
    in_specs = (row_spec, row_spec, seq_spec, seq_spec, P(), P(), P(), P()) + (weight_spec,) * 9 + (cache_spec,) * 4
    out_specs = (P(None, batch_axes), cache_spec, cache_spec)
    return jax.shard_map(local_step, mesh=mesh, in_specs=in_specs, out_specs=out_specs, check_vma=False)
```

```python
import functools

import jax
import jax.numpy as jnp
from jax import lax
from jax.experimental import pallas as pl
from jax.experimental.pallas import tpu as pltpu
from jax.sharding import PartitionSpec as P

NORM_EPS = 1e-6
BUCKET_EDGES = (16, 19, 21, 24, 27, 31, 35, 40, 46, 52, 59, 67, 77, 87, 99, 113)
BUCKET_STARTS = tuple(range(16)) + BUCKET_EDGES
F32 = jnp.float32
BF16 = jnp.bfloat16
LAYERS = 2
SEQS = 2
TOK = 4
COLS = 4
ROWS = 4
PEERS = 16
D = 1024
HEADS = 16
T = 1024
E = 512
FB = 704
FS = 176
REPS = 4
NEG = float("-inf")

SCHEDULE = {
    0: (('z', 0, 1), ('z', 0, 3), ('y', 0, 0), ('in', 0, 0, (0, 2))),
    1: (('y', 0, 1), ('y', 0, 3), ('in', 0, 0, (1, 3))),
    2: (('z', 0, 2), ('in', 0, 1, (0, 2)), ('y', 1, 0)),
    3: (('y', 0, 2), ('in', 0, 1, (1, 3)), ('z', 1, 1), ('z', 1, 3)),
    4: (('x', 0), ('y', 1, 1), ('y', 1, 3), ('z', 1, 2)),
    5: (('y', 1, 2), ('y', 2, 0), ('z', 2, 1), ('z', 2, 3)),
    100: (('e', 0), ('y', 2, 1), ('y', 2, 3), ('z', 2, 2), ('x', 1)),
    8: (('y', 2, 2), ('y', 3, 0), ('z', 3, 1), ('z', 3, 3)),
    9: (('y', 3, 1), ('y', 3, 3), ('x', 2), ('z', 3, 2)),
    10: (('y', 3, 2), ('in', 1, 0, (0, 2)), ('e', 1)),
    20: (('x', 3), ('in', 1, 0, (1, 3)), ('e', 2)),
    21: (('e', 3), ('in', 1, 1, (0, 2)), ('in', 1, 1, (1, 3))),
}


def nt_dot(a, b):
    return lax.dot_general(a, b, (((1,), (1,)), ((), ())), preferred_element_type=F32)


def nn_dot(a, b):
    return jnp.dot(a, b, preferred_element_type=F32)


def body(h0_ref, h1_ref, pos_ref, len_ref, bias_ref, gs_ref, gc_ref, gm_ref,
         wq_hbm, wk_hbm, wv_hbm, wo_hbm, wcq_hbm, wco_hbm, wg_hbm, wu_hbm, wd_hbm,
         sk_hbm, sv_hbm, ck_hbm, cv_hbm,
         hid_ref, new_ref,
         sk, sv, ck, cv, self_bias, proj_w, gate_w, up_w, down_w,
         a_send, a_recv, p3_send, p3_recv, p1_send, p1_recv,
         n_send, n_recv, u_send, u_recv,
         rep, rep_send, rep_recv, cache_sem, weight_sem, mlp_send_sem, mlp_recv_sem, u_send_sem, u_recv_sem, send_sem, recv_sem):
    col = lax.axis_index('col')
    row = lax.axis_index('row')
    me = col * ROWS + row
    dp = lax.axis_index('dp')

    def peer_of(k):
        other = lax.rem(me + k, PEERS)
        return other, other // ROWS, lax.rem(other, ROWS)

    weight_copies = []
    for i, src in enumerate((wq_hbm, wk_hbm, wv_hbm, wo_hbm, wcq_hbm, wco_hbm)):
        cp = pltpu.make_async_copy(src, proj_w.at[i], weight_sem.at[i])
        cp.start()
        weight_copies.append(cp)
    cp = pltpu.make_async_copy(wd_hbm, down_w, weight_sem.at[6])
    cp.start()
    weight_copies.append(cp)
    cache_copies = []
    for l in range(LAYERS):
        for i, (src, dst) in enumerate(((sk_hbm, sk), (sv_hbm, sv), (ck_hbm, ck), (cv_hbm, cv))):
            cp = pltpu.make_async_copy(src.at[l], dst.at[l], cache_sem.at[l, i])
            cp.start()
            cache_copies.append(cp)

    barrier = pltpu.get_barrier_semaphore()
    for k in range(1, PEERS):
        _, c, r = peer_of(k)
        pl.semaphore_signal(barrier, inc=1, device_id={'col': c, 'row': r}, device_id_type=pl.DeviceIdType.MESH)
    pl.semaphore_signal(barrier, inc=1, device_id={'dp': 1 - dp}, device_id_type=pl.DeviceIdType.MESH)
    pl.semaphore_wait(barrier, PEERS)

    def exchange(send, recv, idx, by_row):
        def pick(r, other):
            return 0 if by_row is None else (r if by_row else other)

        for k in range(1, PEERS):
            other, c, r = peer_of(k)
            pltpu.make_async_remote_copy(
                src_ref=send.at[pick(r, other)], dst_ref=recv.at[me],
                send_sem=send_sem.at[idx], recv_sem=recv_sem.at[idx],
                device_id={'col': c, 'row': r}, device_id_type=pl.DeviceIdType.MESH).start()
        recv[me] = send[pick(row, me)]

    def arrive(recv, idx):
        part = recv.at[pl.ds(0, PEERS - 1)]
        pltpu.make_async_copy(part, part, recv_sem.at[idx]).wait()

    def left(recv, idx):
        part = recv.at[pl.ds(0, PEERS - 1)]
        pltpu.make_async_copy(part, part, send_sem.at[idx]).wait()

    def build_bias():
        jpos = lax.broadcasted_iota(jnp.int32, (HEADS, T), 1)
        for b in range(SEQS):
            p = pos_ref[b]
            for t in range(2):
                dist = p + t - jpos
                val = jnp.broadcast_to(bias_ref[:, 0:1], (HEADS, T))
                for n in range(1, 32):
                    val = jnp.where(dist >= BUCKET_STARTS[n], bias_ref[:, n:n + 1], val)
                self_bias[b, pl.ds(t * HEADS, HEADS), :] = jnp.where(jpos < p, val, NEG)

    r32 = lax.broadcasted_iota(jnp.int32, (32, 8), 0)
    c8 = lax.broadcasted_iota(jnp.int32, (32, 8), 1)
    db0 = jnp.concatenate([bias_ref[:, 0:1]] * 2, axis=0)
    db1 = jnp.concatenate([bias_ref[:, 1:2]] * 2, axis=0)
    new_bias = jnp.where(c8 == 0, jnp.where(r32 < HEADS, db0, db1),
                         jnp.where((c8 == 1) & (r32 >= HEADS), db0, NEG))
    head_of = (lax.broadcasted_iota(jnp.int32, (32, D), 1) // 64) == lax.rem(
        lax.broadcasted_iota(jnp.int32, (32, D), 0), HEADS)
    jcross = lax.broadcasted_iota(jnp.int32, (32, E), 1)

    def rms(x, gain):
        mean_sq = jnp.mean(x * x, axis=-1, keepdims=True)
        return x * lax.rsqrt(mean_sq + NORM_EPS) * gain.astype(F32)

    def put_act(vec, l, e):
        for r in range(ROWS):
            a_send[l, e, r] = vec[:, r * 256:(r + 1) * 256]

    def gather_act(recv):
        rows = jnp.concatenate([recv[s].astype(F32) for s in range(PEERS)], axis=0)
        return rows.astype(BF16)

    def spread_query(q4, b):
        q_first = jnp.broadcast_to(q4[b:b + 1, :], (HEADS, D))
        q_second = jnp.broadcast_to(q4[2 + b:3 + b, :], (HEADS, D))
        q = jnp.concatenate([q_first, q_second], axis=0)
        return jnp.where(head_of, q, 0.0).astype(BF16)

    def fold_heads(mixed):
        keep = jnp.where(head_of, mixed, 0.0)
        return (jnp.sum(keep[:HEADS], axis=0, keepdims=True), jnp.sum(keep[HEADS:], axis=0, keepdims=True))

    def join_tokens(pieces):
        return jnp.concatenate([pieces[0][0], pieces[1][0], pieces[0][1], pieces[1][1]], axis=0)

    def row_sum(get):
        return [(get(c * ROWS) + get(c * ROWS + 1)) + (get(c * ROWS + 2) + get(c * ROWS + 3)) for c in range(COLS)]

    def round_bf16(v):
        return v.astype(BF16).astype(F32)

    def project(vec, which, l, e, slot):
        put_act(vec, l, e)
        exchange(a_send.at[l, e], a_recv.at[l, e], l * 10 + slot, True)
        fill(l * 20 + slot)
        arrive(a_recv.at[l, e], l * 10 + slot)
        prod = nn_dot(gather_act(a_recv.at[l, e]), proj_w[which, l])
        for s in range(PEERS):
            p1_send[l, e - 1, s] = prod[s * TOK:(s + 1) * TOK, :]
        exchange(p1_send.at[l, e - 1], p1_recv.at[l, e - 1], l * 10 + slot + 1, False)
        fill(l * 20 + slot + 1)
        arrive(p1_recv.at[l, e - 1], l * 10 + slot + 1)
        sums = row_sum(lambda s: p1_recv[l, e - 1, s])
        return round_bf16(jnp.concatenate(sums, axis=1))

    def mlp_in(l, i, steps):
        src, dst = ((wg_hbm, gate_w), (wu_hbm, up_w))[i]
        for k in steps:
            r = lax.rem(row + k, ROWS)
            part = src.at[l, pl.ds(pl.multiple_of(r * FS, 16), FS), :]
            if k == 0:
                pltpu.make_async_copy(part, dst.at[l, row], mlp_recv_sem.at[l, i]).start()
            else:
                pltpu.make_async_remote_copy(
                    src_ref=part, dst_ref=dst.at[l, row], send_sem=mlp_send_sem.at[l, i],
                    recv_sem=mlp_recv_sem.at[l, i], device_id={'col': col, 'row': r},
                    device_id_type=pl.DeviceIdType.MESH).start()

    def send_u(l):
        for k in range(COLS):
            c = lax.rem(col + k, COLS)

            def away():
                pltpu.make_async_remote_copy(
                    src_ref=u_send.at[l], dst_ref=u_recv.at[l, row], send_sem=u_send_sem.at[l],
                    recv_sem=u_recv_sem.at[l], device_id={'col': c, 'row': col},
                    device_id_type=pl.DeviceIdType.MESH).start()

            if k == 0:
                pl.when(col != row)(away)

                @pl.when(col == row)
                def _():
                    pltpu.make_async_copy(u_send.at[l], u_recv.at[l, row], u_recv_sem.at[l]).start()
            else:
                away()

    own = (wco_hbm.at[0], wo_hbm.at[1], wcq_hbm.at[1], wco_hbm.at[1])
    flip = lax.rem(row + 2, ROWS)
    twin = row + 1 - 2 * lax.rem(row, 2)
    first_row = pl.multiple_of(dp * 128, 128)

    def half(m, j):
        return rep.at[m, j, pl.ds(first_row, 128), :]

    def pass_on(m, step, src, dst, device):
        pltpu.make_async_remote_copy(
            src_ref=src, dst_ref=dst, send_sem=rep_send.at[m], recv_sem=rep_recv.at[m, step],
            device_id=device, device_id_type=pl.DeviceIdType.MESH).start()

    def took(m, step, blocks):
        part = rep.at[m, pl.ds(0, blocks)]
        pltpu.make_async_copy(part, part, rep_recv.at[m, step]).wait()

    def took_halves(m, step, halves):
        part = rep.at[m, pl.ds(0, halves), pl.ds(0, 128), :]
        pltpu.make_async_copy(part, part, rep_recv.at[m, step]).wait()

    def rep_z(m, k):
        if k == 1:
            pltpu.make_async_copy(own[m], rep.at[m, me], rep_recv.at[m, 6]).start()
        pass_on(m, k - 1, own[m].at[pl.ds(first_row, 128), :], half(m, me), {'col': lax.rem(col + k, COLS)})

    def rep_y(m, k):
        j = lax.rem(col + COLS - k, COLS) * ROWS + row
        if k == 0:
            pass_on(m, 3, own[m].at[pl.ds(first_row, 128), :], half(m, j), {'row': flip})
        else:
            took_halves(m, k - 1, 1)
            pass_on(m, 3, half(m, j), half(m, j), {'row': flip})
            pass_on(m, 4, half(m, j), half(m, j), {'dp': 1 - dp})

    def rep_x(m):
        took_halves(m, 3, 4)
        for c in range(COLS):
            j = c * ROWS + flip
            pass_on(m, 4, half(m, j), half(m, j), {'dp': 1 - dp})

    def rep_e(m):
        took_halves(m, 4, 7)
        took(m, 6, 1)
        for c in range(COLS):
            for r in (row, flip):
                j = c * ROWS + r
                pass_on(m, 5, rep.at[m, j], rep.at[m, j], {'row': twin})

    def rep_left(m):
        part = rep.at[m, pl.ds(0, 15)]
        pltpu.make_async_copy(part, part, rep_send.at[m]).wait()

    def local_project(vec, m):
        took(m, 5, 8)
        sums = []
        for c in range(COLS):
            acc = nn_dot(vec[:, 0:256], rep[m, c * ROWS])
            for r in range(1, ROWS):
                acc = acc + nn_dot(vec[:, r * 256:(r + 1) * 256], rep[m, c * ROWS + r])
            sums.append(acc)
        return round_bf16(jnp.concatenate(sums, axis=1))

    work = SCHEDULE

    def fill(slot):
        for name, *what in work.get(slot, ()):
            {'in': mlp_in, 'z': rep_z, 'y': rep_y, 'x': rep_x, 'e': rep_e}[name](*what)

    def mlp_arrive(l):
        for i, dst in enumerate((gate_w, up_w)):
            pltpu.make_async_copy(dst.at[l], dst.at[l], mlp_recv_sem.at[l, i]).wait()

    def mlp_left(l):
        for i, dst in enumerate((gate_w, up_w)):
            part = dst.at[l, pl.ds(0, ROWS - 1)]
            pltpu.make_async_copy(part, part, mlp_send_sem.at[l, i]).wait()
        part = u_recv.at[l, pl.ds(0, COLS - 1)]
        pltpu.make_async_copy(part, part, u_send_sem.at[l]).wait()

        @pl.when(col != row)
        def _():
            pltpu.make_async_copy(u_recv.at[l, 0], u_recv.at[l, 0], u_send_sem.at[l]).wait()

    def apply(vec, which, l, e, slot):
        m = {(0, 5): 0, (1, 3): 1, (1, 4): 2, (1, 5): 3}.get((l, which))
        return project(vec, which, l, e, slot) if m is None else local_project(vec, m)

    x = jnp.concatenate([h0_ref[...].astype(F32), h1_ref[...].astype(F32)], axis=0)
    for l in range(LAYERS):
        base = l * 10
        n = rms(x, gs_ref[l:l + 1, :]).astype(BF16)
        put_act(n, l, 0)
        exchange(a_send.at[l, 0], a_recv.at[l, 0], base, True)
        fill(l * 20)
        if l == 0:
            build_bias()
            for cp in weight_copies:
                cp.wait()
        arrive(a_recv.at[l, 0], base)
        act = gather_act(a_recv.at[l, 0])
        for i in range(3):
            prod = nn_dot(act, proj_w[i, l])
            for s in range(PEERS):
                p3_send[l, s, :, i * 256:(i + 1) * 256] = prod[s * TOK:(s + 1) * TOK, :]
        exchange(p3_send.at[l], p3_recv.at[l], base + 1, False)
        fill(l * 20 + 1)
        arrive(p3_recv.at[l], base + 1)
        sums = row_sum(lambda s: p3_recv[l, s])
        q4, k4, v4 = (round_bf16(jnp.concatenate([sm[:, i * 256:(i + 1) * 256] for sm in sums], axis=1))
                      for i in range(3))
        new_ref[pl.ds(l * 8, TOK), :] = k4
        new_ref[pl.ds(l * 8 + TOK, TOK), :] = v4
        cache_copies[l * 4].wait()
        cache_copies[l * 4 + 1].wait()
        pieces = []
        for b in range(SEQS):
            qb = spread_query(q4, b)
            zeros = jnp.zeros((6, D), F32)
            kn = jnp.concatenate([k4[b:b + 1], k4[2 + b:3 + b], zeros], axis=0).astype(BF16)
            vn = jnp.concatenate([v4[b:b + 1], v4[2 + b:3 + b], zeros], axis=0).astype(BF16)
            old = nn_dot(qb, sk[l, b]) + self_bias[b]
            new = nt_dot(qb, kn) + new_bias
            top = jnp.maximum(jnp.max(old, axis=1, keepdims=True), jnp.max(new, axis=1, keepdims=True))
            e_old = jnp.exp(old - top)
            e_new = jnp.exp(new - top)
            total = jnp.sum(e_old, axis=1, keepdims=True) + jnp.sum(e_new, axis=1, keepdims=True)
            mixed = nt_dot((e_old / total).astype(BF16), sv[l, b]) + nn_dot((e_new / total).astype(BF16), vn)
            pieces.append(fold_heads(mixed))
        x = x + apply(join_tokens(pieces).astype(BF16), 3, l, 1, 2)

        n = rms(x, gc_ref[l:l + 1, :]).astype(BF16)
        q4 = apply(n, 4, l, 2, 4)
        fill(l * 20 + 100)
        cache_copies[l * 4 + 2].wait()
        cache_copies[l * 4 + 3].wait()
        pieces = []
        for b in range(SEQS):
            qb = spread_query(q4, b)
            sc = jnp.where(jcross < len_ref[b], nn_dot(qb, ck[l, b]), NEG)
            ex = jnp.exp(sc - jnp.max(sc, axis=1, keepdims=True))
            probs = (ex / jnp.sum(ex, axis=1, keepdims=True)).astype(BF16)
            pieces.append(fold_heads(nt_dot(probs, cv[l, b])))
        x = x + apply(join_tokens(pieces).astype(BF16), 5, l, 3, 6)

        n_send[l, 0] = rms(x, gm_ref[l:l + 1, :]).astype(BF16)
        exchange(n_send.at[l], n_recv.at[l], base + 8, None)
        fill(l * 20 + 8)
        mlp_arrive(l)
        arrive(n_recv.at[l], base + 8)
        act = gather_act(n_recv.at[l])
        gate = nt_dot(act[:, 0:256], gate_w[l, 0])
        up = nt_dot(act[:, 0:256], up_w[l, 0])
        for r in range(1, ROWS):
            gate = gate + nt_dot(act[:, r * 256:(r + 1) * 256], gate_w[l, r])
            up = up + nt_dot(act[:, r * 256:(r + 1) * 256], up_w[l, r])
        u_send[l] = (jax.nn.silu(round_bf16(gate)) * round_bf16(up)).astype(BF16)
        send_u(l)
        fill(l * 20 + 9)
        pltpu.make_async_copy(u_recv.at[l], u_recv.at[l], u_recv_sem.at[l]).wait()
        prod = nn_dot(u_recv[l, 0], down_w[l, 0:FS])
        for r in range(1, ROWS):
            prod = prod + nn_dot(u_recv[l, r], down_w[l, r * FS:(r + 1) * FS])
        for s in range(PEERS):
            p1_send[l, 3, s] = prod[s * TOK:(s + 1) * TOK, :]
        exchange(p1_send.at[l, 3], p1_recv.at[l, 3], l * 10 + 9, False)
        fill(l * 20 + 10)
        arrive(p1_recv.at[l, 3], l * 10 + 9)
        sums = row_sum(lambda s: p1_recv[l, 3, s])
        x = x + round_bf16(jnp.concatenate(sums, axis=1))

    hid_ref[0] = x[0:2].astype(BF16)
    hid_ref[1] = x[2:4].astype(BF16)
    for l in range(LAYERS):
        base = l * 10
        left(a_recv.at[l, 0], base)
        left(p3_recv.at[l], base + 1)
        for e in (1, 2) if l == 0 else ():
            left(a_recv.at[l, e], base + 2 * e)
            left(p1_recv.at[l, e - 1], base + 2 * e + 1)
        left(n_recv.at[l], base + 8)
        left(p1_recv.at[l, 3], base + 9)
        mlp_left(l)
    for m in range(REPS):
        rep_left(m)


def write_body(pos_ref, new_ref, k_ref, v_ref, ko_ref, vo_ref, cols, patch, sem):
    lanes = lax.broadcasted_iota(jnp.int32, (D, 128), 1)
    blocks = [(l, b, kv) for l in range(LAYERS) for b in range(SEQS) for kv in range(2)]

    def refs(kv):
        return (k_ref, ko_ref) if kv == 0 else (v_ref, vo_ref)

    def tiles(l, b, kv, put):
        first, second = pos_ref[b] // 128, (pos_ref[b] + 1) // 128
        src, dst = refs(kv)
        for i in range(T // 128):
            out = dst.at[l, b, :, pl.ds(i * 128, 128)]
            put(i, first, second, src.at[l, b, :, pl.ds(i * 128, 128)], out)

    for l, b, kv in blocks:
        def plain(i, first, second, src, out):
            @pl.when((first != i) & (second != i))
            def _():
                pltpu.make_async_copy(src, out, sem.at[l, b, kv]).start()

        tiles(l, b, kv, plain)

    cols[...] = jnp.transpose(new_ref[...])
    for l, b, kv in blocks:
        p = pos_ref[b]
        at = l * 8 + kv * TOK + b
        src, _ = refs(kv)
        for q in range(2):
            start = pl.multiple_of(((p + q) // 128) * 128, 128)
            old = src[l, b, :, pl.ds(start, 128)].astype(F32)
            fresh = jnp.where(lanes + start == p, cols[:, at:at + 1],
                              jnp.where(lanes + start == p + 1, cols[:, at + 2:at + 3], old))
            patch[l, b, kv, q] = fresh.astype(BF16)

        def changed(i, first, second, src, out):
            @pl.when(first == i)
            def _():
                pltpu.make_async_copy(patch.at[l, b, kv, 0], out, sem.at[l, b, kv]).start()

            @pl.when((second == i) & (first != i))
            def _():
                pltpu.make_async_copy(patch.at[l, b, kv, 1], out, sem.at[l, b, kv]).start()

        tiles(l, b, kv, changed)
    for l, b, kv in blocks:
        src, dst = refs(kv)
        pltpu.make_async_copy(src.at[l, b], dst.at[l, b], sem.at[l, b, kv]).wait()


def write_caches(pos, new, k, v):
    vmem = pl.BlockSpec(memory_space=pltpu.VMEM)
    return pl.pallas_call(
        write_body,
        out_shape=(jax.ShapeDtypeStruct(k.shape, BF16),) * 2,
        in_specs=[pl.BlockSpec(memory_space=pltpu.SMEM), vmem, vmem, vmem],
        out_specs=(pl.BlockSpec(memory_space=pltpu.HBM),) * 2,
        scratch_shapes=[pltpu.VMEM((D, 16), F32), pltpu.VMEM((LAYERS, SEQS, 2, 2, D, 128), BF16),
                        pltpu.SemaphoreType.DMA((LAYERS, SEQS, 2))],
        compiler_params=pltpu.CompilerParams(vmem_limit_bytes=28 * 1024 * 1024),
        cost_estimate=pl.CostEstimate(flops=1000000, bytes_accessed=32 << 20, transcendentals=0),
    )(pos, new, k, v)


def decode(*args):
    vmem = pl.BlockSpec(memory_space=pltpu.VMEM)
    smem = pl.BlockSpec(memory_space=pltpu.SMEM)
    hbm = pl.BlockSpec(memory_space=pltpu.HBM)
    args = tuple(pltpu.with_memory_space_constraint(a, pltpu.HBM) for a in args)
    return pl.pallas_call(
        body,
        out_shape=(jax.ShapeDtypeStruct((2, SEQS, D), BF16),
                   jax.ShapeDtypeStruct((16, D), F32)),
        in_specs=[vmem, vmem, smem, smem] + [vmem] * 4 + [hbm] * 13,
        out_specs=(vmem,) * 2,
        scratch_shapes=[
            pltpu.VMEM((LAYERS, SEQS, D, T), BF16),
            pltpu.VMEM((LAYERS, SEQS, D, T), BF16),
            pltpu.VMEM((LAYERS, SEQS, D, E), BF16),
            pltpu.VMEM((LAYERS, SEQS, D, E), BF16),
            pltpu.VMEM((SEQS, 32, T), F32),
            pltpu.VMEM((6, LAYERS, 256, 256), BF16),
            pltpu.VMEM((LAYERS, ROWS, FS, 256), BF16),
            pltpu.VMEM((LAYERS, ROWS, FS, 256), BF16),
            pltpu.VMEM((LAYERS, FB, 256), BF16),
            pltpu.VMEM((LAYERS, 4, ROWS, TOK, 256), BF16),
            pltpu.VMEM((LAYERS, 4, PEERS, TOK, 256), BF16),
            pltpu.VMEM((LAYERS, PEERS, TOK, 768), F32),
            pltpu.VMEM((LAYERS, PEERS, TOK, 768), F32),
            pltpu.VMEM((LAYERS, 4, PEERS, TOK, 256), F32),
            pltpu.VMEM((LAYERS, 4, PEERS, TOK, 256), F32),
            pltpu.VMEM((LAYERS, 1, TOK, D), BF16),
            pltpu.VMEM((LAYERS, PEERS, TOK, D), BF16),
            pltpu.VMEM((LAYERS, PEERS * TOK, FS), BF16),
            pltpu.VMEM((LAYERS, ROWS, PEERS * TOK, FS), BF16),
            pltpu.VMEM((REPS, PEERS, 256, 256), BF16),
            pltpu.SemaphoreType.DMA((REPS,)),
            pltpu.SemaphoreType.DMA((REPS, 7)),
            pltpu.SemaphoreType.DMA((LAYERS, 4)),
            pltpu.SemaphoreType.DMA((7,)),
            pltpu.SemaphoreType.DMA((LAYERS, 2)),
            pltpu.SemaphoreType.DMA((LAYERS, 2)),
            pltpu.SemaphoreType.DMA((LAYERS,)),
            pltpu.SemaphoreType.DMA((LAYERS,)),
            pltpu.SemaphoreType.DMA((LAYERS * 10,)),
            pltpu.SemaphoreType.DMA((LAYERS * 10,)),
        ],
        compiler_params=pltpu.CompilerParams(collective_id=0, has_side_effects=True,
                                             vmem_limit_bytes=44 * 1024 * 1024),
        cost_estimate=pl.CostEstimate(flops=400000000, bytes_accessed=32 << 20, transcendentals=0),
    )(*args)


def solution(mesh):
    batch_axes = ('dp', 'col', 'row')

    def local_step(h_first, h_second, start_pos, enc_lens, dec_bias, norm_self, norm_cross, norm_mlp,
                   w_query, w_key, w_value, w_out, w_cquery, w_cout, w_gate, w_up, w_down,
                   self_k, self_v, cross_k, cross_v):
        def flat(cache):
            l, b, t, h, d = cache.shape
            return cache.transpose(0, 1, 3, 4, 2).reshape(l, b, h * d, t)

        def unflat(cache):
            l, b, _, t = cache.shape
            return cache.reshape(l, b, HEADS, 64, t).transpose(0, 1, 4, 2, 3)

        keys, vals = flat(self_k), flat(self_v)
        hidden, new = decode(
            h_first, h_second, start_pos, enc_lens, dec_bias.T, norm_self, norm_cross, norm_mlp,
            w_query, w_key, w_value, w_out, w_cquery, w_cout,
            w_gate.transpose(0, 2, 1), w_up.transpose(0, 2, 1), w_down,
            keys, vals, flat(cross_k), flat(cross_v))
        keys, vals = write_caches(start_pos, new, keys, vals)
        return hidden, unflat(keys), unflat(vals)

    row_spec = P(batch_axes, None)
    seq_spec = P(batch_axes)
    weight_spec = P(None, 'row', 'col')
    cache_spec = P(None, batch_axes)
    in_specs = (row_spec, row_spec, seq_spec, seq_spec, P(), P(), P(), P()) + (weight_spec,) * 9 + (cache_spec,) * 4
    out_specs = (P(None, batch_axes), cache_spec, cache_spec)
    return jax.shard_map(local_step, mesh=mesh, in_specs=in_specs, out_specs=out_specs, check_vma=False)
```

```python
import functools

import jax
import jax.numpy as jnp
from jax import lax
from jax.experimental import pallas as pl
from jax.experimental.pallas import tpu as pltpu
from jax.sharding import PartitionSpec as P

NORM_EPS = 1e-6
BUCKET_EDGES = (16, 19, 21, 24, 27, 31, 35, 40, 46, 52, 59, 67, 77, 87, 99, 113)
BUCKET_STARTS = tuple(range(16)) + BUCKET_EDGES
F32 = jnp.float32
BF16 = jnp.bfloat16
LAYERS = 2
SEQS = 2
TOK = 2
BLK = 256
COLS = 4
ROWS = 4
PEERS = 16
D = 1024
HEADS = 16
T = 1024
E = 512
FB = 704
FS = 176
REPS = 4
PHASES = 4
BESIDE, ACROSS, TWIN, OWN = range(6, 10)
NEG = float("-inf")

SCHEDULE = {
    'n0': 'z01,y00,g00',
    'p0': 'y01,z02,g01',
    'o0': 'y02,z03,g02,z11',
    'r0': 'y03,y11,z12,g03',
    'c0': 'x0,y12,z13,y10,z21',
    'q0': 'y13,y21,z22,y20',
    'k0': 'e0,x1,y22,z23,z31',
    'm0': 'y23,y31,z32,y30',
    'u0': 'x2,y32,z33',
    'd0': 'e1,y33,g10',
    'n1': 'x3,e2,g11',
    'p1': 'e3,g12,g13',
}


def nt_dot(a, b):
    return lax.dot_general(a, b, (((1,), (1,)), ((), ())), preferred_element_type=F32)


def nn_dot(a, b):
    return jnp.dot(a, b, preferred_element_type=F32)


def body(h0_ref, h1_ref, pos_ref, len_ref, bias_ref, gs_ref, gc_ref, gm_ref,
         wq_hbm, wk_hbm, wv_hbm, wo_hbm, wcq_hbm, wco_hbm, wg_hbm, wu_hbm, wd_hbm,
         sk_hbm, sv_hbm, ck_hbm, cv_hbm,
         hid_ref, new_ref,
         sk, sv, ck, cv, self_bias, proj_w, gate_w, up_w, down_w,
         a_send, a_recv, p3_send, p3_recv, p1_send, p1_recv,
         n_send, n_recv, u_send, u_recv,
         rep, rep_send, rep_recv, cache_sem, weight_sem, mlp_send_sem, mlp_recv_sem, u_send_sem, u_recv_sem, send_sem, recv_sem):
    col = lax.axis_index('col')
    row = lax.axis_index('row')
    me = col * ROWS + row
    dp = lax.axis_index('dp')

    def peer_of(k):
        other = lax.rem(me + k, PEERS)
        return other, other // ROWS, lax.rem(other, ROWS)

    weight_copies = []
    for i, src in enumerate((wq_hbm, wk_hbm, wv_hbm, wo_hbm, wcq_hbm, wco_hbm)):
        cp = pltpu.make_async_copy(src, proj_w.at[i], weight_sem.at[i])
        cp.start()
        weight_copies.append(cp)
    cp = pltpu.make_async_copy(wd_hbm, down_w, weight_sem.at[6])
    cp.start()
    weight_copies.append(cp)
    cache_copies = []
    for l in range(LAYERS):
        for i, (src, dst) in enumerate(((sk_hbm, sk), (sv_hbm, sv), (ck_hbm, ck), (cv_hbm, cv))):
            cp = pltpu.make_async_copy(src.at[l], dst.at[l], cache_sem.at[l, i])
            cp.start()
            cache_copies.append(cp)

    barrier = pltpu.get_barrier_semaphore()
    for k in range(1, PEERS):
        _, c, r = peer_of(k)
        pl.semaphore_signal(barrier, inc=1, device_id={'col': c, 'row': r}, device_id_type=pl.DeviceIdType.MESH)
    pl.semaphore_signal(barrier, inc=1, device_id={'dp': 1 - dp}, device_id_type=pl.DeviceIdType.MESH)
    pl.semaphore_wait(barrier, PEERS)

    def exchange(send, recv, idx, by_row):
        def pick(r, other):
            return 0 if by_row is None else (r if by_row else other)

        for k in range(1, PEERS):
            other, c, r = peer_of(k)
            pltpu.make_async_remote_copy(
                src_ref=send.at[pick(r, other)], dst_ref=recv.at[me],
                send_sem=send_sem.at[idx], recv_sem=recv_sem.at[idx],
                device_id={'col': c, 'row': r}, device_id_type=pl.DeviceIdType.MESH).start()
        recv[me] = send[pick(row, me)]

    def arrive(recv, idx):
        part = recv.at[pl.ds(0, PEERS - 1)]
        pltpu.make_async_copy(part, part, recv_sem.at[idx]).wait()

    def left(recv, idx):
        part = recv.at[pl.ds(0, PEERS - 1)]
        pltpu.make_async_copy(part, part, send_sem.at[idx]).wait()

    def build_bias():
        jpos = lax.broadcasted_iota(jnp.int32, (HEADS, T), 1)
        for b in range(SEQS):
            p = pos_ref[b]
            for t in range(2):
                dist = p + t - jpos
                val = jnp.broadcast_to(bias_ref[:, 0:1], (HEADS, T))
                for n in range(1, 32):
                    val = jnp.where(dist >= BUCKET_STARTS[n], bias_ref[:, n:n + 1], val)
                self_bias[b, pl.ds(t * HEADS, HEADS), :] = jnp.where(jpos < p, val, NEG)

    r32 = lax.broadcasted_iota(jnp.int32, (32, 8), 0)
    c8 = lax.broadcasted_iota(jnp.int32, (32, 8), 1)
    db0 = jnp.concatenate([bias_ref[:, 0:1]] * 2, axis=0)
    db1 = jnp.concatenate([bias_ref[:, 1:2]] * 2, axis=0)
    new_bias = jnp.where(c8 == 0, jnp.where(r32 < HEADS, db0, db1),
                         jnp.where((c8 == 1) & (r32 >= HEADS), db0, NEG))
    head_of = (lax.broadcasted_iota(jnp.int32, (32, D), 1) // 64) == lax.rem(
        lax.broadcasted_iota(jnp.int32, (32, D), 0), HEADS)
    jcross = lax.broadcasted_iota(jnp.int32, (32, E), 1)

    def rms(x, gain):
        mean_sq = jnp.mean(x * x, axis=-1, keepdims=True)
        return x * lax.rsqrt(mean_sq + NORM_EPS) * gain.astype(F32)

    def column(vec, r):
        return vec[:, r * BLK:(r + 1) * BLK]

    def rows_of(prod, s):
        return prod[s * TOK:(s + 1) * TOK]

    def put_act(vec, buf):
        for r in range(ROWS):
            buf[r] = column(vec, r)

    def gather_act(recv):
        rows = jnp.concatenate([recv[s].astype(F32) for s in range(PEERS)], axis=0)
        return rows.astype(BF16)

    def spread_query(q):
        both = jnp.concatenate([jnp.broadcast_to(q[t:t + 1, :], (HEADS, D)) for t in range(TOK)], axis=0)
        return jnp.where(head_of, both, 0.0).astype(BF16)

    def fold_heads(mixed):
        keep = jnp.where(head_of, mixed, 0.0)
        return jnp.concatenate([jnp.sum(keep[:HEADS], axis=0, keepdims=True),
                                jnp.sum(keep[HEADS:], axis=0, keepdims=True)], axis=0)

    def row_sum(get):
        return [(get(c * ROWS) + get(c * ROWS + 1)) + (get(c * ROWS + 2) + get(c * ROWS + 3)) for c in range(COLS)]

    def round_bf16(v):
        return v.astype(BF16).astype(F32)

    def project(vec, which, b, l, e, names):
        idx = sem_of(b, l, e)
        put_act(vec, a_send.at[b, l, e])
        exchange(a_send.at[b, l, e], a_recv.at[b, l, e], idx, True)
        yield names[0]
        arrive(a_recv.at[b, l, e], idx)
        prod = nn_dot(gather_act(a_recv.at[b, l, e]), proj_w[which, l])
        yield from back(prod, b, l, e, names[1])
        return back_sum(b, l, e)

    def sem_of(b, l, e):
        return ((b * LAYERS) + l) * 2 * PHASES + 2 * e

    def back(prod, b, l, e, name):
        for s in range(PEERS):
            p1_send[b, l, e, s] = rows_of(prod, s)
        exchange(p1_send.at[b, l, e], p1_recv.at[b, l, e], sem_of(b, l, e) + 1, False)
        yield name
        arrive(p1_recv.at[b, l, e], sem_of(b, l, e) + 1)

    def back_sum(b, l, e):
        return round_bf16(jnp.concatenate(row_sum(lambda s: p1_recv[b, l, e, s]), axis=1))

    def mlp_in(l, share):
        i = share // 2
        src, dst = ((wg_hbm, gate_w), (wu_hbm, up_w))[i]
        for k in range(share % 2, ROWS, 2):
            r = lax.rem(row + k, ROWS)
            part = src.at[l, pl.ds(pl.multiple_of(r * FS, HEADS), FS), :]
            if k == 0:
                pltpu.make_async_copy(part, dst.at[l, row], mlp_recv_sem.at[l, i]).start()
            else:
                pltpu.make_async_remote_copy(
                    src_ref=part, dst_ref=dst.at[l, row], send_sem=mlp_send_sem.at[l, i],
                    recv_sem=mlp_recv_sem.at[l, i], device_id={'col': col, 'row': r},
                    device_id_type=pl.DeviceIdType.MESH).start()

    def send_u(b, l):
        src, dst = u_send.at[b, l], u_recv.at[b, l, row]

        def away(c):
            pltpu.make_async_remote_copy(
                src_ref=src, dst_ref=dst, send_sem=u_send_sem.at[b, l], recv_sem=u_recv_sem.at[b, l],
                device_id={'col': c, 'row': col}, device_id_type=pl.DeviceIdType.MESH).start()

        for k in range(1, COLS):
            away(lax.rem(col + k, COLS))

        @pl.when(col != row)
        def _():
            away(col)

        @pl.when(col == row)
        def _():
            pltpu.make_async_copy(src, dst, u_recv_sem.at[b, l]).start()

    own = (wco_hbm.at[0], wo_hbm.at[1], wcq_hbm.at[1], wco_hbm.at[1])
    flip = lax.rem(row + 2, ROWS)
    twin = row + 1 - 2 * lax.rem(row, 2)
    first_row = pl.multiple_of(dp * 128, 128)

    def half(m, j):
        return rep.at[m, j, pl.ds(first_row, 128), :]

    def pass_on(m, step, src, dst, device):
        pltpu.make_async_remote_copy(
            src_ref=src, dst_ref=dst, send_sem=rep_send.at[m], recv_sem=rep_recv.at[m, step],
            device_id=device, device_id_type=pl.DeviceIdType.MESH).start()

    def took(m, step, blocks):
        part = rep.at[m, pl.ds(0, blocks)]
        pltpu.make_async_copy(part, part, rep_recv.at[m, step]).wait()

    def took_halves(m, step, halves):
        part = rep.at[m, pl.ds(0, halves), pl.ds(0, 128), :]
        pltpu.make_async_copy(part, part, rep_recv.at[m, step]).wait()

    def own_half(m):
        return own[m].at[pl.ds(first_row, 128), :]

    def rep_z(m, t):
        if t == 1:
            pltpu.make_async_copy(own[m], rep.at[m, me], rep_recv.at[m, OWN]).start()
        for way, (there, plane, onward) in enumerate((
                ((col >= t - 1) & (col < COLS - 1), col - (t - 1), col + 1),
                ((col + t <= COLS) & (col > 0), col + (t - 1), col - 1))):
            @pl.when(there)
            def _():
                j = plane * ROWS + row
                src = own_half(m) if t == 1 else half(m, j)
                pass_on(m, way * 3 + t - 1, src, half(m, j), {'col': onward})

    def rep_y(m, t):
        if t == 0:
            pass_on(m, BESIDE, own_half(m), half(m, me), {'row': flip})
            return
        for way, (there, plane) in enumerate(((col >= t, col - t), (col + t < COLS, col + t))):
            @pl.when(there)
            def _():
                j = plane * ROWS + row
                took_halves(m, way * 3 + t - 1, 1)
                pass_on(m, BESIDE, half(m, j), half(m, j), {'row': flip})
                pass_on(m, ACROSS, half(m, j), half(m, j), {'dp': 1 - dp})

    def rep_x(m):
        took_halves(m, BESIDE, COLS)
        for c in range(COLS):
            j = c * ROWS + flip
            pass_on(m, ACROSS, half(m, j), half(m, j), {'dp': 1 - dp})

    def rep_e(m):
        took_halves(m, ACROSS, 2 * COLS - 1)
        took(m, OWN, 1)
        for c in range(COLS):
            for r in (row, flip):
                j = c * ROWS + r
                pass_on(m, TWIN, rep.at[m, j], rep.at[m, j], {'row': twin})

    def rep_left(m):
        def gone(part):
            pltpu.make_async_copy(part, part, rep_send.at[m]).wait()

        gone(rep.at[m, pl.ds(0, 2 * COLS)])
        gone(rep.at[m, pl.ds(0, 3 * COLS - 1), pl.ds(0, 128), :])
        for t in range(1, COLS):
            for there in ((col >= t - 1) & (col < COLS - 1), (col + t <= COLS) & (col > 0)):
                @pl.when(there)
                def _():
                    gone(rep.at[m, 0, pl.ds(0, 128), :])

    def add_up(terms):
        return functools.reduce(jnp.add, terms)

    def local_project(vec, m, b):
        if b == 0:
            took(m, TWIN, 2 * COLS)
        sums = []
        for c in range(COLS):
            sums.append(add_up([nn_dot(column(vec, r), rep[m, c * ROWS + r]) for r in range(ROWS)]))
        return round_bf16(jnp.concatenate(sums, axis=1))

    def fill(name):
        for item in SCHEDULE.get(name, '').split(','):
            if item:
                move = {'g': mlp_in, 'z': rep_z, 'y': rep_y, 'x': rep_x, 'e': rep_e}[item[0]]
                move(*[int(digit) for digit in item[1:]])

    def mlp_arrive(l):
        for i, dst in enumerate((gate_w, up_w)):
            pltpu.make_async_copy(dst.at[l], dst.at[l], mlp_recv_sem.at[l, i]).wait()

    def mlp_left(l):
        for i, dst in enumerate((gate_w, up_w)):
            part = dst.at[l, pl.ds(0, ROWS - 1)]
            pltpu.make_async_copy(part, part, mlp_send_sem.at[l, i]).wait()
        for b in range(SEQS):
            part = u_recv.at[b, l, pl.ds(0, COLS - 1)]
            pltpu.make_async_copy(part, part, u_send_sem.at[b, l]).wait()

            @pl.when(col != row)
            def _():
                one = u_recv.at[b, l, 0]
                pltpu.make_async_copy(one, one, u_send_sem.at[b, l]).wait()

    whole = {'o0': None, 'c0': None, 'k0': 0, 'o1': 1, 'c1': 2, 'k1': 3}

    def apply(vec, which, b, l, e, names):
        m = whole[names[0]]
        if m is None:
            return (yield from project(vec, which, b, l, e, names))
        return local_project(vec, m, b)

    def self_attention(q, k, v, b, l):
        qb = spread_query(q)
        zeros = jnp.zeros((8 - TOK, D), F32)
        kn = jnp.concatenate([k, zeros], axis=0).astype(BF16)
        vn = jnp.concatenate([v, zeros], axis=0).astype(BF16)
        old = nn_dot(qb, sk[l, b]) + self_bias[b]
        new = nt_dot(qb, kn) + new_bias
        top = jnp.maximum(jnp.max(old, axis=1, keepdims=True), jnp.max(new, axis=1, keepdims=True))
        e_old = jnp.exp(old - top)
        e_new = jnp.exp(new - top)
        total = jnp.sum(e_old, axis=1, keepdims=True) + jnp.sum(e_new, axis=1, keepdims=True)
        mixed = nt_dot((e_old / total).astype(BF16), sv[l, b]) + nn_dot((e_new / total).astype(BF16), vn)
        return fold_heads(mixed).astype(BF16)

    def cross_attention(q, b, l):
        sc = jnp.where(jcross < len_ref[b], nn_dot(spread_query(q), ck[l, b]), NEG)
        ex = jnp.exp(sc - jnp.max(sc, axis=1, keepdims=True))
        probs = (ex / jnp.sum(ex, axis=1, keepdims=True)).astype(BF16)
        return fold_heads(nt_dot(probs, cv[l, b])).astype(BF16)

    def stream(b, done):
        x = jnp.concatenate([h[b:b + 1].astype(F32) for h in (h0_ref, h1_ref)], axis=0)
        for l in range(LAYERS):
            idx = sem_of(b, l, 0)
            put_act(rms(x, gs_ref[l:l + 1, :]).astype(BF16), a_send.at[b, l, 0])
            exchange(a_send.at[b, l, 0], a_recv.at[b, l, 0], idx, True)
            yield f'n{l}'
            arrive(a_recv.at[b, l, 0], idx)
            act = gather_act(a_recv.at[b, l, 0])
            for i in range(3):
                prod = nn_dot(act, proj_w[i, l])
                for s in range(PEERS):
                    p3_send[b, l, s, :, i * BLK:(i + 1) * BLK] = rows_of(prod, s)
            exchange(p3_send.at[b, l], p3_recv.at[b, l], idx + 1, False)
            yield f'p{l}'
            arrive(p3_recv.at[b, l], idx + 1)
            sums = row_sum(lambda s: p3_recv[b, l, s])
            q, k, v = (round_bf16(jnp.concatenate([column(sm, i) for sm in sums], axis=1)) for i in range(3))
            for kv, fresh in enumerate((k, v)):
                new_ref[pl.ds(((l * 2 + kv) * SEQS + b) * TOK, TOK), :] = fresh
            if b == 0:
                cache_copies[l * 4].wait()
                cache_copies[l * 4 + 1].wait()
            x = x + (yield from apply(self_attention(q, k, v, b, l), 3, b, l, 1, (f'o{l}', f'r{l}')))

            n = rms(x, gc_ref[l:l + 1, :]).astype(BF16)
            q = yield from apply(n, 4, b, l, 2, (f'c{l}', f'q{l}'))
            if b == 0:
                fill(f'k{l}')
                cache_copies[l * 4 + 2].wait()
                cache_copies[l * 4 + 3].wait()
            x = x + (yield from apply(cross_attention(q, b, l), 5, b, l, 3, (f'k{l}', '')))

            n_send[b, l, 0] = rms(x, gm_ref[l:l + 1, :]).astype(BF16)
            idx = sem_of(b, l, 3)
            exchange(n_send.at[b, l], n_recv.at[b, l], idx, None)
            yield f'm{l}'
            if b == 0:
                mlp_arrive(l)
            arrive(n_recv.at[b, l], idx)
            act = gather_act(n_recv.at[b, l])
            gate, up = (add_up([nt_dot(column(act, r), w[l, r]) for r in range(ROWS)]) for w in (gate_w, up_w))
            u_send[b, l] = (jax.nn.silu(round_bf16(gate)) * round_bf16(up)).astype(BF16)
            send_u(b, l)
            yield f'u{l}'
            pltpu.make_async_copy(u_recv.at[b, l], u_recv.at[b, l], u_recv_sem.at[b, l]).wait()
            prod = add_up([nn_dot(u_recv[b, l, r], down_w[l, r * FS:(r + 1) * FS]) for r in range(ROWS)])
            yield from back(prod, b, l, 3, f'd{l}')
            x = x + back_sum(b, l, 3)
        done.append(x)

    done = []
    streams = [stream(b, done) for b in range(SEQS)]
    while True:
        names = [next(streams[0], '')]
        if not names[0]:
            next(streams[1], '')
            break
        fill(names[0])
        next(streams[1], '')
        if names[0] == 'n0':
            build_bias()
            for cp in weight_copies:
                cp.wait()
    for t in range(TOK):
        hid_ref[t] = jnp.concatenate([x[t:t + 1] for x in done], axis=0).astype(BF16)
    for l in range(LAYERS):
        for b in range(SEQS):
            left(a_recv.at[b, l, 0], sem_of(b, l, 0))
            left(p3_recv.at[b, l], sem_of(b, l, 0) + 1)
            for e in range(1, 3 - 2 * l):
                left(a_recv.at[b, l, e], sem_of(b, l, e))
                left(p1_recv.at[b, l, e], sem_of(b, l, e) + 1)
            left(n_recv.at[b, l], sem_of(b, l, 3))
            left(p1_recv.at[b, l, 3], sem_of(b, l, 3) + 1)
        mlp_left(l)
    for m in range(REPS):
        rep_left(m)


def write_body(pos_ref, new_ref, k_ref, v_ref, ko_ref, vo_ref, cols, patch, sem):
    lanes = lax.broadcasted_iota(jnp.int32, (D, 128), 1)
    blocks = [(l, b, kv) for l in range(LAYERS) for b in range(SEQS) for kv in range(2)]

    def refs(kv):
        return (k_ref, ko_ref) if kv == 0 else (v_ref, vo_ref)

    def tiles(l, b, kv, put):
        first, second = pos_ref[b] // 128, (pos_ref[b] + 1) // 128
        src, dst = refs(kv)
        for i in range(T // 128):
            out = dst.at[l, b, :, pl.ds(i * 128, 128)]
            put(i, first, second, src.at[l, b, :, pl.ds(i * 128, 128)], out)

    for l, b, kv in blocks:
        def plain(i, first, second, src, out):
            @pl.when((first != i) & (second != i))
            def _():
                pltpu.make_async_copy(src, out, sem.at[l, b, kv]).start()

        tiles(l, b, kv, plain)

    cols[...] = jnp.transpose(new_ref[...])
    for l, b, kv in blocks:
        p = pos_ref[b]
        at = ((l * 2 + kv) * SEQS + b) * TOK
        src, _ = refs(kv)
        for q in range(2):
            start = pl.multiple_of(((p + q) // 128) * 128, 128)
            old = src[l, b, :, pl.ds(start, 128)].astype(F32)
            fresh = jnp.where(lanes + start == p, cols[:, at:at + 1],
                              jnp.where(lanes + start == p + 1, cols[:, at + 1:at + 2], old))
            patch[l, b, kv, q] = fresh.astype(BF16)

        def changed(i, first, second, src, out):
            @pl.when(first == i)
            def _():
                pltpu.make_async_copy(patch.at[l, b, kv, 0], out, sem.at[l, b, kv]).start()

            @pl.when((second == i) & (first != i))
            def _():
                pltpu.make_async_copy(patch.at[l, b, kv, 1], out, sem.at[l, b, kv]).start()

        tiles(l, b, kv, changed)
    for l, b, kv in blocks:
        src, dst = refs(kv)
        pltpu.make_async_copy(src.at[l, b], dst.at[l, b], sem.at[l, b, kv]).wait()


def write_caches(pos, new, k, v):
    vmem = pl.BlockSpec(memory_space=pltpu.VMEM)
    return pl.pallas_call(
        write_body,
        out_shape=(jax.ShapeDtypeStruct(k.shape, BF16),) * 2,
        in_specs=[pl.BlockSpec(memory_space=pltpu.SMEM), vmem, vmem, vmem],
        out_specs=(pl.BlockSpec(memory_space=pltpu.HBM),) * 2,
        scratch_shapes=[pltpu.VMEM((D, 16), F32), pltpu.VMEM((LAYERS, SEQS, 2, 2, D, 128), BF16),
                        pltpu.SemaphoreType.DMA((LAYERS, SEQS, 2))],
        compiler_params=pltpu.CompilerParams(vmem_limit_bytes=28 * 1024 * 1024),
        cost_estimate=pl.CostEstimate(flops=1000000, bytes_accessed=32 << 20, transcendentals=0),
    )(pos, new, k, v)


def decode(*args):
    both = (SEQS, LAYERS)
    vmem = pl.BlockSpec(memory_space=pltpu.VMEM)
    smem = pl.BlockSpec(memory_space=pltpu.SMEM)
    hbm = pl.BlockSpec(memory_space=pltpu.HBM)
    args = tuple(pltpu.with_memory_space_constraint(a, pltpu.HBM) for a in args)
    return pl.pallas_call(
        body,
        out_shape=(jax.ShapeDtypeStruct((2, SEQS, D), BF16),
                   jax.ShapeDtypeStruct((16, D), F32)),
        in_specs=[vmem, vmem, smem, smem] + [vmem] * 4 + [hbm] * 13,
        out_specs=(vmem,) * 2,
        scratch_shapes=[
            pltpu.VMEM((LAYERS, SEQS, D, T), BF16),
            pltpu.VMEM((LAYERS, SEQS, D, T), BF16),
            pltpu.VMEM((LAYERS, SEQS, D, E), BF16),
            pltpu.VMEM((LAYERS, SEQS, D, E), BF16),
            pltpu.VMEM((SEQS, 32, T), F32),
            pltpu.VMEM((6, LAYERS, 256, 256), BF16),
            pltpu.VMEM((LAYERS, ROWS, FS, 256), BF16),
            pltpu.VMEM((LAYERS, ROWS, FS, 256), BF16),
            pltpu.VMEM((LAYERS, FB, 256), BF16),
            pltpu.VMEM(both + (3, ROWS, TOK, BLK), BF16),
            pltpu.VMEM(both + (3, PEERS, TOK, BLK), BF16),
            pltpu.VMEM(both + (PEERS, TOK, 3 * BLK), F32),
            pltpu.VMEM(both + (PEERS, TOK, 3 * BLK), F32),
            pltpu.VMEM(both + (PHASES, PEERS, TOK, BLK), F32),
            pltpu.VMEM(both + (PHASES, PEERS, TOK, BLK), F32),
            pltpu.VMEM(both + (1, TOK, D), BF16),
            pltpu.VMEM(both + (PEERS, TOK, D), BF16),
            pltpu.VMEM(both + (PEERS * TOK, FS), BF16),
            pltpu.VMEM(both + (ROWS, PEERS * TOK, FS), BF16),
            pltpu.VMEM((REPS, PEERS, 256, 256), BF16),
            pltpu.SemaphoreType.DMA((REPS,)),
            pltpu.SemaphoreType.DMA((REPS, OWN + 1)),
            pltpu.SemaphoreType.DMA((LAYERS, 4)),
            pltpu.SemaphoreType.DMA((7,)),
            pltpu.SemaphoreType.DMA((LAYERS, 2)),
            pltpu.SemaphoreType.DMA((LAYERS, 2)),
            pltpu.SemaphoreType.DMA(both),
            pltpu.SemaphoreType.DMA(both),
            pltpu.SemaphoreType.DMA((SEQS * LAYERS * 2 * PHASES,)),
            pltpu.SemaphoreType.DMA((SEQS * LAYERS * 2 * PHASES,)),
        ],
        compiler_params=pltpu.CompilerParams(collective_id=0, has_side_effects=True,
                                             vmem_limit_bytes=44 * 1024 * 1024),
        cost_estimate=pl.CostEstimate(flops=400000000, bytes_accessed=32 << 20, transcendentals=0),
    )(*args)


def solution(mesh):
    batch_axes = ('dp', 'col', 'row')

    def local_step(h_first, h_second, start_pos, enc_lens, dec_bias, norm_self, norm_cross, norm_mlp,
                   w_query, w_key, w_value, w_out, w_cquery, w_cout, w_gate, w_up, w_down,
                   self_k, self_v, cross_k, cross_v):
        def flat(cache):
            l, b, t, h, d = cache.shape
            return cache.transpose(0, 1, 3, 4, 2).reshape(l, b, h * d, t)

        def unflat(cache):
            l, b, _, t = cache.shape
            return cache.reshape(l, b, HEADS, 64, t).transpose(0, 1, 4, 2, 3)

        keys, vals = flat(self_k), flat(self_v)
        hidden, new = decode(
            h_first, h_second, start_pos, enc_lens, dec_bias.T, norm_self, norm_cross, norm_mlp,
            w_query, w_key, w_value, w_out, w_cquery, w_cout,
            w_gate.transpose(0, 2, 1), w_up.transpose(0, 2, 1), w_down,
            keys, vals, flat(cross_k), flat(cross_v))
        keys, vals = write_caches(start_pos, new, keys, vals)
        return hidden, unflat(keys), unflat(vals)

    row_spec = P(batch_axes, None)
    seq_spec = P(batch_axes)
    weight_spec = P(None, 'row', 'col')
    cache_spec = P(None, batch_axes)
    in_specs = (row_spec, row_spec, seq_spec, seq_spec, P(), P(), P(), P()) + (weight_spec,) * 9 + (cache_spec,) * 4
    out_specs = (P(None, batch_axes), cache_spec, cache_spec)
    return jax.shard_map(local_step, mesh=mesh, in_specs=in_specs, out_specs=out_specs, check_vma=False)
```

```python
import functools

import jax
import jax.numpy as jnp
from jax import lax
from jax.experimental import pallas as pl
from jax.experimental.pallas import tpu as pltpu
from jax.sharding import PartitionSpec as P

NORM_EPS = 1e-6
BUCKET_EDGES = (16, 19, 21, 24, 27, 31, 35, 40, 46, 52, 59, 67, 77, 87, 99, 113)
BUCKET_STARTS = tuple(range(16)) + BUCKET_EDGES
F32 = jnp.float32
BF16 = jnp.bfloat16
LAYERS = 2
SEQS = 2
TOK = 2
BLK = 256
COLS = 4
ROWS = 4
PEERS = 16
D = 1024
HEADS = 16
T = 1024
E = 512
FB = 704
FS = 176
REPS = 4
PHASES = 4
BESIDE, ACROSS, TWIN, OWN = range(6, 10)
NEG = float("-inf")

SCHEDULE = {
    'n0': 'z01,y00,g00',
    'p0': 'y01,z02,g01',
    'o0': 'y02,z03,g02,z11',
    'r0': 'y03,y11,z12,g03',
    'c0': 'x0,y12,z13,y10,z21',
    'q0': 'y13,y21,z22,y20',
    'k0': 'e0,x1,y22,z23,z31',
    'm0': 'y23,y31,z32,y30',
    'u0': 'x2,y32,z33',
    'd0': 'e1,y33,g10',
    'n1': 'x3,e2,g11',
    'p1': 'e3,g12,g13',
}


def nt_dot(a, b):
    return lax.dot_general(a, b, (((1,), (1,)), ((), ())), preferred_element_type=F32)


def nn_dot(a, b):
    return jnp.dot(a, b, preferred_element_type=F32)


def body(h0_ref, h1_ref, pos_ref, len_ref, bias_ref, gs_ref, gc_ref, gm_ref,
         wq_hbm, wk_hbm, wv_hbm, wo_hbm, wcq_hbm, wco_hbm, wg_hbm, wu_hbm, wd_hbm,
         sk_hbm, sv_hbm, ck_hbm, cv_hbm,
         hid_ref, new_ref,
         sk, sv, ck, cv, self_bias, proj_w, gate_w, up_w, down_w,
         a_send, a_recv, p3_send, p3_recv, p1_send, p1_recv,
         n_send, n_recv, u_send, u_recv,
         rep, rep_send, rep_recv, cache_sem, weight_sem, mlp_send_sem, mlp_recv_sem, u_send_sem, u_recv_sem, send_sem, recv_sem):
    col = lax.axis_index('col')
    row = lax.axis_index('row')
    me = col * ROWS + row
    dp = lax.axis_index('dp')

    def peer_of(k):
        other = lax.rem(me + k, PEERS)
        return other, other // ROWS, lax.rem(other, ROWS)

    weight_copies = []
    for i, src in enumerate((wq_hbm, wk_hbm, wv_hbm, wo_hbm, wcq_hbm, wco_hbm)):
        cp = pltpu.make_async_copy(src, proj_w.at[i], weight_sem.at[i])
        cp.start()
        weight_copies.append(cp)
    cp = pltpu.make_async_copy(wd_hbm, down_w, weight_sem.at[6])
    cp.start()
    weight_copies.append(cp)
    cache_copies = []
    for l in range(LAYERS):
        for i, (src, dst) in enumerate(((sk_hbm, sk), (sv_hbm, sv), (ck_hbm, ck), (cv_hbm, cv))):
            cp = pltpu.make_async_copy(src.at[l], dst.at[l], cache_sem.at[l, i])
            cp.start()
            cache_copies.append(cp)

    barrier = pltpu.get_barrier_semaphore()
    for k in range(1, PEERS):
        _, c, r = peer_of(k)
        pl.semaphore_signal(barrier, inc=1, device_id={'col': c, 'row': r}, device_id_type=pl.DeviceIdType.MESH)
    pl.semaphore_signal(barrier, inc=1, device_id={'dp': 1 - dp}, device_id_type=pl.DeviceIdType.MESH)
    pl.semaphore_wait(barrier, PEERS)

    def exchange(send, recv, idx, by_row):
        def pick(r, other):
            return 0 if by_row is None else (r if by_row else other)

        for k in sorted(range(1, PEERS), key=lambda k: abs(2 * k - PEERS)):
            other, c, r = peer_of(k)
            pltpu.make_async_remote_copy(
                src_ref=send.at[pick(r, other)], dst_ref=recv.at[me],
                send_sem=send_sem.at[idx], recv_sem=recv_sem.at[idx],
                device_id={'col': c, 'row': r}, device_id_type=pl.DeviceIdType.MESH).start()
        recv[me] = send[pick(row, me)]

    def arrive(recv, idx):
        part = recv.at[pl.ds(0, PEERS - 1)]
        pltpu.make_async_copy(part, part, recv_sem.at[idx]).wait()

    def left(recv, idx):
        part = recv.at[pl.ds(0, PEERS - 1)]
        pltpu.make_async_copy(part, part, send_sem.at[idx]).wait()

    def build_bias():
        jpos = lax.broadcasted_iota(jnp.int32, (HEADS, T), 1)
        for b in range(SEQS):
            p = pos_ref[b]
            for t in range(2):
                dist = p + t - jpos
                val = jnp.broadcast_to(bias_ref[:, 0:1], (HEADS, T))
                for n in range(1, 32):
                    val = jnp.where(dist >= BUCKET_STARTS[n], bias_ref[:, n:n + 1], val)
                self_bias[b, pl.ds(t * HEADS, HEADS), :] = jnp.where(jpos < p, val, NEG)

    r32 = lax.broadcasted_iota(jnp.int32, (32, 8), 0)
    c8 = lax.broadcasted_iota(jnp.int32, (32, 8), 1)
    db0 = jnp.concatenate([bias_ref[:, 0:1]] * 2, axis=0)
    db1 = jnp.concatenate([bias_ref[:, 1:2]] * 2, axis=0)
    new_bias = jnp.where(c8 == 0, jnp.where(r32 < HEADS, db0, db1),
                         jnp.where((c8 == 1) & (r32 >= HEADS), db0, NEG))
    head_of = (lax.broadcasted_iota(jnp.int32, (32, D), 1) // 64) == lax.rem(
        lax.broadcasted_iota(jnp.int32, (32, D), 0), HEADS)
    jcross = lax.broadcasted_iota(jnp.int32, (32, E), 1)

    def rms(x, gain):
        mean_sq = jnp.mean(x * x, axis=-1, keepdims=True)
        return x * lax.rsqrt(mean_sq + NORM_EPS) * gain.astype(F32)

    def column(vec, r):
        return vec[:, r * BLK:(r + 1) * BLK]

    def rows_of(prod, s):
        return prod[s * TOK:(s + 1) * TOK]

    def put_act(vec, buf):
        for r in range(ROWS):
            buf[r] = column(vec, r)

    def gather_act(recv):
        rows = jnp.concatenate([recv[s].astype(F32) for s in range(PEERS)], axis=0)
        return rows.astype(BF16)

    def spread_query(q):
        both = jnp.concatenate([jnp.broadcast_to(q[t:t + 1, :], (HEADS, D)) for t in range(TOK)], axis=0)
        return jnp.where(head_of, both, 0.0).astype(BF16)

    def fold_heads(mixed):
        keep = jnp.where(head_of, mixed, 0.0)
        return jnp.concatenate([jnp.sum(keep[:HEADS], axis=0, keepdims=True),
                                jnp.sum(keep[HEADS:], axis=0, keepdims=True)], axis=0)

    def row_sum(get):
        return [(get(c * ROWS) + get(c * ROWS + 1)) + (get(c * ROWS + 2) + get(c * ROWS + 3)) for c in range(COLS)]

    def round_bf16(v):
        return v.astype(BF16).astype(F32)

    def project(vec, which, b, l, e, names):
        idx = sem_of(b, l, e)
        put_act(vec, a_send.at[b, l, e])
        exchange(a_send.at[b, l, e], a_recv.at[b, l, e], idx, True)
        yield names[0]
        arrive(a_recv.at[b, l, e], idx)
        prod = nn_dot(gather_act(a_recv.at[b, l, e]), proj_w[which, l])
        yield from back(prod, b, l, e, names[1])
        return back_sum(b, l, e)

    def sem_of(b, l, e):
        return ((b * LAYERS) + l) * 2 * PHASES + 2 * e

    def back(prod, b, l, e, name):
        for s in range(PEERS):
            p1_send[b, l, e, s] = rows_of(prod, s)
        exchange(p1_send.at[b, l, e], p1_recv.at[b, l, e], sem_of(b, l, e) + 1, False)
        yield name
        arrive(p1_recv.at[b, l, e], sem_of(b, l, e) + 1)

    def back_sum(b, l, e):
        return round_bf16(jnp.concatenate(row_sum(lambda s: p1_recv[b, l, e, s]), axis=1))

    def mlp_in(l, share):
        i = share // 2
        src, dst = ((wg_hbm, gate_w), (wu_hbm, up_w))[i]
        for k in range(share % 2, ROWS, 2):
            r = lax.rem(row + k, ROWS)
            part = src.at[l, pl.ds(pl.multiple_of(r * FS, HEADS), FS), :]
            if k == 0:
                pltpu.make_async_copy(part, dst.at[l, row], mlp_recv_sem.at[l, i]).start()
            else:
                pltpu.make_async_remote_copy(
                    src_ref=part, dst_ref=dst.at[l, row], send_sem=mlp_send_sem.at[l, i],
                    recv_sem=mlp_recv_sem.at[l, i], device_id={'col': col, 'row': r},
                    device_id_type=pl.DeviceIdType.MESH).start()

    def send_u(b, l):
        src, dst = u_send.at[b, l], u_recv.at[b, l, row]

        def away(c):
            pltpu.make_async_remote_copy(
                src_ref=src, dst_ref=dst, send_sem=u_send_sem.at[b, l], recv_sem=u_recv_sem.at[b, l],
                device_id={'col': c, 'row': col}, device_id_type=pl.DeviceIdType.MESH).start()

        for k in range(1, COLS):
            away(lax.rem(col + k, COLS))

        @pl.when(col != row)
        def _():
            away(col)

        @pl.when(col == row)
        def _():
            pltpu.make_async_copy(src, dst, u_recv_sem.at[b, l]).start()

    own = (wco_hbm.at[0], wo_hbm.at[1], wcq_hbm.at[1], wco_hbm.at[1])
    flip = lax.rem(row + 2, ROWS)
    twin = row + 1 - 2 * lax.rem(row, 2)
    first_row = pl.multiple_of(dp * 128, 128)

    def half(m, j):
        return rep.at[m, j, pl.ds(first_row, 128), :]

    def pass_on(m, step, src, dst, device):
        pltpu.make_async_remote_copy(
            src_ref=src, dst_ref=dst, send_sem=rep_send.at[m], recv_sem=rep_recv.at[m, step],
            device_id=device, device_id_type=pl.DeviceIdType.MESH).start()

    def took(m, step, blocks):
        part = rep.at[m, pl.ds(0, blocks)]
        pltpu.make_async_copy(part, part, rep_recv.at[m, step]).wait()

    def took_halves(m, step, halves):
        part = rep.at[m, pl.ds(0, halves), pl.ds(0, 128), :]
        pltpu.make_async_copy(part, part, rep_recv.at[m, step]).wait()

    def own_half(m):
        return own[m].at[pl.ds(first_row, 128), :]

    def rep_z(m, t):
        if t == 1:
            pltpu.make_async_copy(own[m], rep.at[m, me], rep_recv.at[m, OWN]).start()
        for way, (there, plane, onward) in enumerate((
                ((col >= t - 1) & (col < COLS - 1), col - (t - 1), col + 1),
                ((col + t <= COLS) & (col > 0), col + (t - 1), col - 1))):
            @pl.when(there)
            def _():
                j = plane * ROWS + row
                src = own_half(m) if t == 1 else half(m, j)
                pass_on(m, way * 3 + t - 1, src, half(m, j), {'col': onward})

    def rep_y(m, t):
        if t == 0:
            pass_on(m, BESIDE, own_half(m), half(m, me), {'row': flip})
            return
        for way, (there, plane) in enumerate(((col >= t, col - t), (col + t < COLS, col + t))):
            @pl.when(there)
            def _():
                j = plane * ROWS + row
                took_halves(m, way * 3 + t - 1, 1)
                pass_on(m, BESIDE, half(m, j), half(m, j), {'row': flip})
                pass_on(m, ACROSS, half(m, j), half(m, j), {'dp': 1 - dp})

    def rep_x(m):
        took_halves(m, BESIDE, COLS)
        for c in range(COLS):
            j = c * ROWS + flip
            pass_on(m, ACROSS, half(m, j), half(m, j), {'dp': 1 - dp})

    def rep_e(m):
        took_halves(m, ACROSS, 2 * COLS - 1)
        took(m, OWN, 1)
        for c in range(COLS):
            for r in (row, flip):
                j = c * ROWS + r
                pass_on(m, TWIN, rep.at[m, j], rep.at[m, j], {'row': twin})

    def rep_left(m):
        def gone(part):
            pltpu.make_async_copy(part, part, rep_send.at[m]).wait()

        gone(rep.at[m, pl.ds(0, 2 * COLS)])
        gone(rep.at[m, pl.ds(0, 3 * COLS - 1), pl.ds(0, 128), :])
        for t in range(1, COLS):
            for there in ((col >= t - 1) & (col < COLS - 1), (col + t <= COLS) & (col > 0)):
                @pl.when(there)
                def _():
                    gone(rep.at[m, 0, pl.ds(0, 128), :])

    def add_up(terms):
        return functools.reduce(jnp.add, terms)

    def local_project(vec, m, b):
        if b == 0:
            took(m, TWIN, 2 * COLS)
        sums = []
        for c in range(COLS):
            sums.append(add_up([nn_dot(column(vec, r), rep[m, c * ROWS + r]) for r in range(ROWS)]))
        return round_bf16(jnp.concatenate(sums, axis=1))

    def fill(name):
        for item in SCHEDULE.get(name, '').split(','):
            if item:
                move = {'g': mlp_in, 'z': rep_z, 'y': rep_y, 'x': rep_x, 'e': rep_e}[item[0]]
                move(*[int(digit) for digit in item[1:]])

    def mlp_arrive(l):
        for i, dst in enumerate((gate_w, up_w)):
            pltpu.make_async_copy(dst.at[l], dst.at[l], mlp_recv_sem.at[l, i]).wait()

    def mlp_left(l):
        for i, dst in enumerate((gate_w, up_w)):
            part = dst.at[l, pl.ds(0, ROWS - 1)]
            pltpu.make_async_copy(part, part, mlp_send_sem.at[l, i]).wait()
        for b in range(SEQS):
            part = u_recv.at[b, l, pl.ds(0, COLS - 1)]
            pltpu.make_async_copy(part, part, u_send_sem.at[b, l]).wait()

            @pl.when(col != row)
            def _():
                one = u_recv.at[b, l, 0]
                pltpu.make_async_copy(one, one, u_send_sem.at[b, l]).wait()

    whole = {'o0': None, 'c0': None, 'k0': 0, 'o1': 1, 'c1': 2, 'k1': 3}

    def apply(vec, which, b, l, e, names):
        m = whole[names[0]]
        if m is None:
            return (yield from project(vec, which, b, l, e, names))
        return local_project(vec, m, b)

    def self_attention(q, k, v, b, l):
        qb = spread_query(q)
        zeros = jnp.zeros((8 - TOK, D), F32)
        kn = jnp.concatenate([k, zeros], axis=0).astype(BF16)
        vn = jnp.concatenate([v, zeros], axis=0).astype(BF16)
        old = nn_dot(qb, sk[l, b]) + self_bias[b]
        new = nt_dot(qb, kn) + new_bias
        top = jnp.maximum(jnp.max(old, axis=1, keepdims=True), jnp.max(new, axis=1, keepdims=True))
        e_old = jnp.exp(old - top)
        e_new = jnp.exp(new - top)
        total = jnp.sum(e_old, axis=1, keepdims=True) + jnp.sum(e_new, axis=1, keepdims=True)
        mixed = nt_dot((e_old / total).astype(BF16), sv[l, b]) + nn_dot((e_new / total).astype(BF16), vn)
        return fold_heads(mixed).astype(BF16)

    def cross_attention(q, b, l):
        sc = jnp.where(jcross < len_ref[b], nn_dot(spread_query(q), ck[l, b]), NEG)
        ex = jnp.exp(sc - jnp.max(sc, axis=1, keepdims=True))
        probs = (ex / jnp.sum(ex, axis=1, keepdims=True)).astype(BF16)
        return fold_heads(nt_dot(probs, cv[l, b])).astype(BF16)

    def stream(b, done):
        x = jnp.concatenate([h[b:b + 1].astype(F32) for h in (h0_ref, h1_ref)], axis=0)
        for l in range(LAYERS):
            idx = sem_of(b, l, 0)
            put_act(rms(x, gs_ref[l:l + 1, :]).astype(BF16), a_send.at[b, l, 0])
            exchange(a_send.at[b, l, 0], a_recv.at[b, l, 0], idx, True)
            yield f'n{l}'
            arrive(a_recv.at[b, l, 0], idx)
            act = gather_act(a_recv.at[b, l, 0])
            for i in range(3):
                prod = nn_dot(act, proj_w[i, l])
                for s in range(PEERS):
                    p3_send[b, l, s, :, i * BLK:(i + 1) * BLK] = rows_of(prod, s)
            exchange(p3_send.at[b, l], p3_recv.at[b, l], idx + 1, False)
            yield f'p{l}'
            arrive(p3_recv.at[b, l], idx + 1)
            sums = row_sum(lambda s: p3_recv[b, l, s])
            q, k, v = (round_bf16(jnp.concatenate([column(sm, i) for sm in sums], axis=1)) for i in range(3))
            for kv, fresh in enumerate((k, v)):
                new_ref[pl.ds(((l * 2 + kv) * SEQS + b) * TOK, TOK), :] = fresh
            if b == 0:
                cache_copies[l * 4].wait()
                cache_copies[l * 4 + 1].wait()
            x = x + (yield from apply(self_attention(q, k, v, b, l), 3, b, l, 1, (f'o{l}', f'r{l}')))

            n = rms(x, gc_ref[l:l + 1, :]).astype(BF16)
            q = yield from apply(n, 4, b, l, 2, (f'c{l}', f'q{l}'))
            if b == 0:
                fill(f'k{l}')
                cache_copies[l * 4 + 2].wait()
                cache_copies[l * 4 + 3].wait()
            x = x + (yield from apply(cross_attention(q, b, l), 5, b, l, 3, (f'k{l}', '')))

            n_send[b, l, 0] = rms(x, gm_ref[l:l + 1, :]).astype(BF16)
            idx = sem_of(b, l, 3)
            exchange(n_send.at[b, l], n_recv.at[b, l], idx, None)
            yield f'm{l}'
            if b == 0:
                mlp_arrive(l)
            arrive(n_recv.at[b, l], idx)
            act = gather_act(n_recv.at[b, l])
            gate, up = (add_up([nt_dot(column(act, r), w[l, r]) for r in range(ROWS)]) for w in (gate_w, up_w))
            u_send[b, l] = (jax.nn.silu(round_bf16(gate)) * round_bf16(up)).astype(BF16)
            send_u(b, l)
            yield f'u{l}'
            pltpu.make_async_copy(u_recv.at[b, l], u_recv.at[b, l], u_recv_sem.at[b, l]).wait()
            prod = add_up([nn_dot(u_recv[b, l, r], down_w[l, r * FS:(r + 1) * FS]) for r in range(ROWS)])
            yield from back(prod, b, l, 3, f'd{l}')
            x = x + back_sum(b, l, 3)
        done.append(x)

    done = []
    streams = [stream(b, done) for b in range(SEQS)]
    while True:
        names = [next(streams[0], '')]
        if not names[0]:
            next(streams[1], '')
            break
        late = names[0][0] in 'npm'
        if not late:
            fill(names[0])
        next(streams[1], '')
        if late:
            fill(names[0])
        if names[0] == 'n0':
            build_bias()
            for cp in weight_copies:
                cp.wait()
    for t in range(TOK):
        hid_ref[t] = jnp.concatenate([x[t:t + 1] for x in done], axis=0).astype(BF16)
    for l in range(LAYERS):
        for b in range(SEQS):
            left(a_recv.at[b, l, 0], sem_of(b, l, 0))
            left(p3_recv.at[b, l], sem_of(b, l, 0) + 1)
            for e in range(1, 3 - 2 * l):
                left(a_recv.at[b, l, e], sem_of(b, l, e))
                left(p1_recv.at[b, l, e], sem_of(b, l, e) + 1)
            left(n_recv.at[b, l], sem_of(b, l, 3))
            left(p1_recv.at[b, l, 3], sem_of(b, l, 3) + 1)
        mlp_left(l)
    for m in range(REPS):
        rep_left(m)


def write_body(pos_ref, new_ref, k_ref, v_ref, ko_ref, vo_ref, cols, patch, sem):
    lanes = lax.broadcasted_iota(jnp.int32, (D, 128), 1)
    blocks = [(l, b, kv) for l in range(LAYERS) for b in range(SEQS) for kv in range(2)]

    def refs(kv):
        return (k_ref, ko_ref) if kv == 0 else (v_ref, vo_ref)

    def tiles(l, b, kv, put):
        first, second = pos_ref[b] // 128, (pos_ref[b] + 1) // 128
        src, dst = refs(kv)
        for i in range(T // 128):
            out = dst.at[l, b, :, pl.ds(i * 128, 128)]
            put(i, first, second, src.at[l, b, :, pl.ds(i * 128, 128)], out)

    for l, b, kv in blocks:
        def plain(i, first, second, src, out):
            @pl.when((first != i) & (second != i))
            def _():
                pltpu.make_async_copy(src, out, sem.at[l, b, kv]).start()

        tiles(l, b, kv, plain)

    cols[...] = jnp.transpose(new_ref[...])
    for l, b, kv in blocks:
        p = pos_ref[b]
        at = ((l * 2 + kv) * SEQS + b) * TOK
        src, _ = refs(kv)
        for q in range(2):
            start = pl.multiple_of(((p + q) // 128) * 128, 128)
            old = src[l, b, :, pl.ds(start, 128)].astype(F32)
            fresh = jnp.where(lanes + start == p, cols[:, at:at + 1],
                              jnp.where(lanes + start == p + 1, cols[:, at + 1:at + 2], old))
            patch[l, b, kv, q] = fresh.astype(BF16)

        def changed(i, first, second, src, out):
            @pl.when(first == i)
            def _():
                pltpu.make_async_copy(patch.at[l, b, kv, 0], out, sem.at[l, b, kv]).start()

            @pl.when((second == i) & (first != i))
            def _():
                pltpu.make_async_copy(patch.at[l, b, kv, 1], out, sem.at[l, b, kv]).start()

        tiles(l, b, kv, changed)
    for l, b, kv in blocks:
        src, dst = refs(kv)
        pltpu.make_async_copy(src.at[l, b], dst.at[l, b], sem.at[l, b, kv]).wait()


def write_caches(pos, new, k, v):
    vmem = pl.BlockSpec(memory_space=pltpu.VMEM)
    return pl.pallas_call(
        write_body,
        out_shape=(jax.ShapeDtypeStruct(k.shape, BF16),) * 2,
        in_specs=[pl.BlockSpec(memory_space=pltpu.SMEM), vmem, vmem, vmem],
        out_specs=(pl.BlockSpec(memory_space=pltpu.HBM),) * 2,
        scratch_shapes=[pltpu.VMEM((D, 16), F32), pltpu.VMEM((LAYERS, SEQS, 2, 2, D, 128), BF16),
                        pltpu.SemaphoreType.DMA((LAYERS, SEQS, 2))],
        compiler_params=pltpu.CompilerParams(vmem_limit_bytes=28 * 1024 * 1024),
        cost_estimate=pl.CostEstimate(flops=1000000, bytes_accessed=32 << 20, transcendentals=0),
    )(pos, new, k, v)


def decode(*args):
    both = (SEQS, LAYERS)
    vmem = pl.BlockSpec(memory_space=pltpu.VMEM)
    smem = pl.BlockSpec(memory_space=pltpu.SMEM)
    hbm = pl.BlockSpec(memory_space=pltpu.HBM)
    args = tuple(pltpu.with_memory_space_constraint(a, pltpu.HBM) for a in args)
    return pl.pallas_call(
        body,
        out_shape=(jax.ShapeDtypeStruct((2, SEQS, D), BF16),
                   jax.ShapeDtypeStruct((16, D), F32)),
        in_specs=[vmem, vmem, smem, smem] + [vmem] * 4 + [hbm] * 13,
        out_specs=(vmem,) * 2,
        scratch_shapes=[
            pltpu.VMEM((LAYERS, SEQS, D, T), BF16),
            pltpu.VMEM((LAYERS, SEQS, D, T), BF16),
            pltpu.VMEM((LAYERS, SEQS, D, E), BF16),
            pltpu.VMEM((LAYERS, SEQS, D, E), BF16),
            pltpu.VMEM((SEQS, 32, T), F32),
            pltpu.VMEM((6, LAYERS, 256, 256), BF16),
            pltpu.VMEM((LAYERS, ROWS, FS, 256), BF16),
            pltpu.VMEM((LAYERS, ROWS, FS, 256), BF16),
            pltpu.VMEM((LAYERS, FB, 256), BF16),
            pltpu.VMEM(both + (3, ROWS, TOK, BLK), BF16),
            pltpu.VMEM(both + (3, PEERS, TOK, BLK), BF16),
            pltpu.VMEM(both + (PEERS, TOK, 3 * BLK), F32),
            pltpu.VMEM(both + (PEERS, TOK, 3 * BLK), F32),
            pltpu.VMEM(both + (PHASES, PEERS, TOK, BLK), F32),
            pltpu.VMEM(both + (PHASES, PEERS, TOK, BLK), F32),
            pltpu.VMEM(both + (1, TOK, D), BF16),
            pltpu.VMEM(both + (PEERS, TOK, D), BF16),
            pltpu.VMEM(both + (PEERS * TOK, FS), BF16),
            pltpu.VMEM(both + (ROWS, PEERS * TOK, FS), BF16),
            pltpu.VMEM((REPS, PEERS, 256, 256), BF16),
            pltpu.SemaphoreType.DMA((REPS,)),
            pltpu.SemaphoreType.DMA((REPS, OWN + 1)),
            pltpu.SemaphoreType.DMA((LAYERS, 4)),
            pltpu.SemaphoreType.DMA((7,)),
            pltpu.SemaphoreType.DMA((LAYERS, 2)),
            pltpu.SemaphoreType.DMA((LAYERS, 2)),
            pltpu.SemaphoreType.DMA(both),
            pltpu.SemaphoreType.DMA(both),
            pltpu.SemaphoreType.DMA((SEQS * LAYERS * 2 * PHASES,)),
            pltpu.SemaphoreType.DMA((SEQS * LAYERS * 2 * PHASES,)),
        ],
        compiler_params=pltpu.CompilerParams(collective_id=0, has_side_effects=True,
                                             vmem_limit_bytes=44 * 1024 * 1024),
        cost_estimate=pl.CostEstimate(flops=400000000, bytes_accessed=32 << 20, transcendentals=0),
    )(*args)


def solution(mesh):
    batch_axes = ('dp', 'col', 'row')

    def local_step(h_first, h_second, start_pos, enc_lens, dec_bias, norm_self, norm_cross, norm_mlp,
                   w_query, w_key, w_value, w_out, w_cquery, w_cout, w_gate, w_up, w_down,
                   self_k, self_v, cross_k, cross_v):
        def flat(cache):
            l, b, t, h, d = cache.shape
            return cache.transpose(0, 1, 3, 4, 2).reshape(l, b, h * d, t)

        def unflat(cache):
            l, b, _, t = cache.shape
            return cache.reshape(l, b, HEADS, 64, t).transpose(0, 1, 4, 2, 3)

        keys, vals = flat(self_k), flat(self_v)
        hidden, new = decode(
            h_first, h_second, start_pos, enc_lens, dec_bias.T, norm_self, norm_cross, norm_mlp,
            w_query, w_key, w_value, w_out, w_cquery, w_cout,
            w_gate.transpose(0, 2, 1), w_up.transpose(0, 2, 1), w_down,
            keys, vals, flat(cross_k), flat(cross_v))
        keys, vals = write_caches(start_pos, new, keys, vals)
        return hidden, unflat(keys), unflat(vals)

    row_spec = P(batch_axes, None)
    seq_spec = P(batch_axes)
    weight_spec = P(None, 'row', 'col')
    cache_spec = P(None, batch_axes)
    in_specs = (row_spec, row_spec, seq_spec, seq_spec, P(), P(), P(), P()) + (weight_spec,) * 9 + (cache_spec,) * 4
    out_specs = (P(None, batch_axes), cache_spec, cache_spec)
    return jax.shard_map(local_step, mesh=mesh, in_specs=in_specs, out_specs=out_specs, check_vma=False)
```
